32 devices in a mesh: tm: 4 (over x, core), space: 8 (over z, y).
Axes of the slice: x: 2, y: 2, z: 4, core: 2. Of those that a mesh axis runs over, the one named last changes fastest.
Arguments:
- iterate: float32 [64, 16, 3, 4096], P('space', 'tm'), may hold values from -6 to 6
- forcing: float32 [64, 16, 3, 4096], P('space', 'tm'), may hold values from -6 to 6
- initial_velocity: float32 [64, 3, 4096], P('space'), may hold values from -6 to 6
- viscosity: float32 [64, 4096], P('space'), may hold values from 0.1 to 1
- peclet: float32 [64, 3, 4096], P('space'), may hold values from -0.9 to 0.9
- live_patch_mask: int32 [64], P('space'), may hold values from 0 to 1, as said below
- neighbour_holder: int32 [64, 6], P('space'), may hold values from -1 to 7, as said below
- neighbour_slot: int32 [64, 6], P('space'), may hold values from -1 to 7, as said below
Outputs:
- corrected_velocity: float32 [64, 16, 3, 4096], P('space', 'tm')
- corrected_residual: float32 [64, 16, 3, 4096], P('space', 'tm')
The draws below stay inside these ranges and needn't reach their ends.
Inputs may be any that keep to these rules, and one draw needn't show every extreme that they name: `live_patch_mask`: on each index of space the live slots (1) come first; their count is 2 to 8, and in every draw some two indices j and j + 4 have all 8 slots live. `neighbour_holder`: the patches of one index s of space are the blocks of one aligned 2x2x2 octant; the octant's position is read from the bits of s: bit b of s is bit b div 3 of coordinate b mod 3, except that where a coordinate has two bits its lower bit is complemented when its higher bit is 1; slot p lies at offsets (p mod 2, p div 2 mod 2, p div 4); the entry is -1 where no live patch lies across the face or the slot is dead; the relation is symmetric across opposite faces; the live patches of one index face those of another given index across at most 4 faces, exactly 4 for some pair in every draw. `neighbour_slot`: -1 exactly where neighbour_holder is -1.
All inputs are finite; a program needn't handle non-finite values.
Results may differ from the reference program's by a relative error of at most 0.0003.
Values sent between devices are 32-bit elements; how exact they have to be, the bound alone decides.
A program may use at most 192 MiB of HBM per device.

```python
import math
from functools import partial
import jax
import jax.numpy as jnp
from jax import lax

WINDOW_SLICES = 16
BLOCK_EDGE = 16
SLOTS_PER_SPACE = 8
SWEEPS = 5
TOTAL_SLOTS = 64
BLOCK_CELLS = 4096


def octant_layout(key):
    key = jax.random.fold_in(key, 7919)
    count_key, pair_key = jax.random.split(key)
    space_members = TOTAL_SLOTS // SLOTS_PER_SPACE
    levels = max(space_members - 1, 1).bit_length()
    half_members = max(space_members // 2, 1)
    counts = jax.random.randint(count_key, (space_members,), 2, 7)
    chosen = jax.random.randint(pair_key, (), 0, half_members)
    if space_members >= 16:
        chosen = jnp.bitwise_or(chosen, 1)
    device_ids = jnp.arange(space_members, dtype=jnp.int32)
    counts = jnp.where(device_ids % half_members == chosen, SLOTS_PER_SPACE, counts).astype(jnp.int32)
    slot_numbers = jnp.arange(TOTAL_SLOTS, dtype=jnp.int32)
    holders = slot_numbers // SLOTS_PER_SPACE
    local_slot = slot_numbers % SLOTS_PER_SPACE
    octant = [jnp.zeros_like(slot_numbers), jnp.zeros_like(slot_numbers), jnp.zeros_like(slot_numbers)]
    extents = [2, 2, 2]
    coord_bits = [0, 0, 0]
    for bit_index in range(levels):
        octant[bit_index % 3] = octant[bit_index % 3] + ((holders >> bit_index & 1) << bit_index // 3)
        extents[bit_index % 3] = extents[bit_index % 3] * 2
        coord_bits[bit_index % 3] = coord_bits[bit_index % 3] + 1
    for axis_id in range(3):
        if coord_bits[axis_id] == 2:
            octant[axis_id] = jnp.bitwise_xor(octant[axis_id], octant[axis_id] >> 1 & 1)
    coords = [2 * octant[axis_id] + (local_slot >> axis_id & 1) for axis_id in range(3)]
    live_self = local_slot < counts[holders]
    owner_columns = []
    slot_columns = []
    for face_id in range(6):
        axis_id = face_id // 2
        shifted = list(coords)
        shifted[axis_id] = coords[axis_id] + (2 * (face_id % 2) - 1)
        inside = (shifted[axis_id] >= 0) & (shifted[axis_id] < extents[axis_id])
        clipped = [jnp.clip(shifted[other_axis], 0, extents[other_axis] - 1) for other_axis in range(3)]
        decoded = []
        for other_axis in range(3):
            value = clipped[other_axis] // 2
            if coord_bits[other_axis] == 2:
                value = jnp.bitwise_xor(value, value >> 1 & 1)
            decoded.append(value)
        octant_code = jnp.zeros_like(slot_numbers)
        for bit_index in range(levels):
            octant_code = octant_code + ((decoded[bit_index % 3] >> bit_index // 3 & 1) << bit_index)
        neighbour_local = (clipped[0] & 1) + ((clipped[1] & 1) << 1) + ((clipped[2] & 1) << 2)
        in_range = octant_code < space_members
        safe_code = jnp.minimum(octant_code, space_members - 1)
        present = inside & in_range & live_self & (neighbour_local < counts[safe_code])
        owner_columns.append(jnp.where(present, octant_code, -1))
        slot_columns.append(jnp.where(present, neighbour_local, -1))
    live_mask = live_self.astype(jnp.int32)
    return (live_mask, jnp.stack(owner_columns, axis=1).astype(jnp.int32), jnp.stack(slot_columns, axis=1).astype(jnp.int32))


def draw_live_patch_mask(key, part):
    return octant_layout(key)[0]


def draw_neighbour_holder(key, part):
    return octant_layout(key)[1]


def draw_neighbour_slot(key, part):
    return octant_layout(key)[2]


def steps_of(rng, shape, cuts, low, largest):
    level = 1.0
    for dim, parts in cuts:
        draws = jax.random.uniform(jax.random.fold_in(jax.random.fold_in(rng, 6), dim), (parts,), jnp.float32, low / len(cuts), largest / len(cuts))
        level = level * jnp.repeat(jnp.exp(draws), shape[dim] // parts).reshape((-1,) + (1,) * (len(shape) - 1 - dim))
    return level


def centred(stream_key, dims, scale, limit, cuts=(), kind=jnp.bfloat16):
    result = jax.random.normal(stream_key, dims, jnp.float32) * scale
    if len(cuts) > 0:
        result = steps_of(stream_key, dims, cuts, -0.22, 0.18) * result
    return jnp.clip(result, min=-limit, max=limit).astype(kind)


def setup_inputs(seed: int = 0) -> dict:
    seeds = jax.random.split(jax.random.key(seed), 9)
    return {
        "iterate": centred(seeds[0], (TOTAL_SLOTS, WINDOW_SLICES, 3, BLOCK_CELLS), 1.0, 6.0, ((0, 8), (1, 4)), jnp.float32),
        "forcing": centred(seeds[1], (TOTAL_SLOTS, WINDOW_SLICES, 3, BLOCK_CELLS), 1.0, 6.0, ((0, 8), (1, 4)), jnp.float32),
        "initial_velocity": centred(seeds[2], (TOTAL_SLOTS, 3, BLOCK_CELLS), 1.0, 6.0, ((0, 8),), jnp.float32),
        "viscosity": jnp.clip(jnp.exp(math.log(1.0) - 2.3025851 * jax.random.uniform(seeds[3], (TOTAL_SLOTS, BLOCK_CELLS), jnp.float32) ** steps_of(seeds[3], (TOTAL_SLOTS, BLOCK_CELLS), ((0, 8),), -0.2, 0.2)), 0.1, 1.0),
        "peclet": jnp.clip(jax.random.uniform(seeds[4], (TOTAL_SLOTS, 3, BLOCK_CELLS), jnp.float32, -0.9, 0.9) * steps_of(seeds[4], (TOTAL_SLOTS, 3, BLOCK_CELLS), ((0, 8),), -0.4, 0.0), -0.9, 0.9),
        "live_patch_mask": draw_live_patch_mask(jax.random.fold_in(seeds[8], 71), 0),
        "neighbour_holder": draw_neighbour_holder(jax.random.fold_in(seeds[8], 71), 0),
        "neighbour_slot": draw_neighbour_slot(jax.random.fold_in(seeds[8], 71), 0),
    }


STEP_DURATION = 0.5
ALPHA_SCALE = 0.1
HIGHEST_PRECISION = lax.Precision.HIGHEST


def face_layers(block_shaped):
    return jnp.stack([block_shaped[:, :, 0], block_shaped[:, :, -1], block_shaped[:, :, :, 0], block_shaped[:, :, :, -1], block_shaped[:, :, :, :, 0], block_shaped[:, :, :, :, -1]], axis=1)


def across_faces(block_shaped, neighbour_holder, neighbour_slot):
    patch_count = block_shaped.shape[0]
    channels = block_shaped.shape[1]
    layers = face_layers(block_shaped).reshape(patch_count * 6, channels, BLOCK_EDGE, BLOCK_EDGE)
    opposite = jnp.array([1, 0, 3, 2, 5, 4], dtype=jnp.int32)
    source = (jnp.maximum(neighbour_holder, 0) * SLOTS_PER_SPACE + jnp.maximum(neighbour_slot, 0)) * 6 + opposite[None, :]
    gathered = jnp.take(layers, source.reshape(-1).astype(jnp.int32), axis=0).reshape(patch_count, 6, channels, BLOCK_EDGE, BLOCK_EDGE)
    present = (neighbour_holder >= 0) & (neighbour_slot >= 0)
    return jnp.where(present[:, :, None, None, None], gathered, jnp.zeros_like(gathered))


def adjacent_total(block_shaped, ghost_faces, peclet_shaped):
    padded = jnp.pad(block_shaped, ((0, 0), (0, 0), (1, 1), (1, 1), (1, 1)))
    padded = padded.at[:, :, 0, 1:-1, 1:-1].set(ghost_faces[:, 0])
    padded = padded.at[:, :, -1, 1:-1, 1:-1].set(ghost_faces[:, 1])
    padded = padded.at[:, :, 1:-1, 0, 1:-1].set(ghost_faces[:, 2])
    padded = padded.at[:, :, 1:-1, -1, 1:-1].set(ghost_faces[:, 3])
    padded = padded.at[:, :, 1:-1, 1:-1, 0].set(ghost_faces[:, 4])
    padded = padded.at[:, :, 1:-1, 1:-1, -1].set(ghost_faces[:, 5])
    x_peclet = peclet_shaped[:, 0:1]
    y_peclet = peclet_shaped[:, 1:2]
    z_peclet = peclet_shaped[:, 2:3]
    summed = (1.0 - x_peclet) * padded[:, :, 2:, 1:-1, 1:-1] + (1.0 + x_peclet) * padded[:, :, :-2, 1:-1, 1:-1]
    summed = summed + (1.0 - y_peclet) * padded[:, :, 1:-1, 2:, 1:-1] + (1.0 + y_peclet) * padded[:, :, 1:-1, :-2, 1:-1]
    summed = summed + (1.0 - z_peclet) * padded[:, :, 1:-1, 1:-1, 2:] + (1.0 + z_peclet) * padded[:, :, 1:-1, 1:-1, :-2]
    return summed


def residual_grid(velocity_state, forcing_history, initial_velocity, viscosity, peclet_shaped, live_indicator, neighbour_holder, neighbour_slot):
    earlier = jnp.concatenate([initial_velocity[None], velocity_state[:-1]], axis=0)

    def one_slice(pieces):
        present_iterate, prior_velocity, right_hand_side = pieces
        block_shaped = present_iterate.reshape(TOTAL_SLOTS, 3, BLOCK_EDGE, BLOCK_EDGE, BLOCK_EDGE)
        ghost_faces = across_faces(block_shaped, neighbour_holder, neighbour_slot)
        adjacent_sum = adjacent_total(block_shaped, ghost_faces, peclet_shaped).reshape(TOTAL_SLOTS, 3, BLOCK_EDGE ** 3)
        operator_result = viscosity[:, None, :] * (6.0 * present_iterate - adjacent_sum)
        return (right_hand_side - (present_iterate - prior_velocity) / STEP_DURATION - operator_result) * live_indicator[:, None, None]

    return lax.map(one_slice, (velocity_state, earlier, forcing_history))


def solve_frequency(pieces, viscosity, peclet_shaped, neighbour_holder, neighbour_slot):
    source_real, source_imag, shift_real, shift_imag = pieces
    diagonal = shift_real + 6.0 * viscosity[:, None, :]
    determinant = diagonal * diagonal + shift_imag * shift_imag
    real_component = jnp.zeros_like(source_real)
    imaginary_component = jnp.zeros_like(source_imag)
    for sweep_index in range(SWEEPS):
        stacked_slices = jnp.stack([real_component, imaginary_component], axis=1).reshape(TOTAL_SLOTS, 6, BLOCK_EDGE, BLOCK_EDGE, BLOCK_EDGE)
        ghost_faces = across_faces(stacked_slices, neighbour_holder, neighbour_slot)
        adjacent_sum = adjacent_total(stacked_slices, ghost_faces, peclet_shaped).reshape(TOTAL_SLOTS, 2, 3, BLOCK_EDGE ** 3)
        total_real = source_real + viscosity[:, None, :] * adjacent_sum[:, 0]
        total_imag = source_imag + viscosity[:, None, :] * adjacent_sum[:, 1]
        real_component = (diagonal * total_real + shift_imag * total_imag) / determinant
        imaginary_component = (diagonal * total_imag - shift_imag * total_real) / determinant
    return real_component, imaginary_component


def reference(iterate, forcing, initial_velocity, viscosity, peclet, live_patch_mask, neighbour_holder, neighbour_slot):
    velocity_state = jnp.transpose(iterate, (1, 0, 2, 3))
    forcing_history = jnp.transpose(forcing, (1, 0, 2, 3))
    live_indicator = live_patch_mask.astype(jnp.float32)
    peclet_shaped = peclet.reshape(TOTAL_SLOTS, 3, BLOCK_EDGE, BLOCK_EDGE, BLOCK_EDGE)
    residual_value = residual_grid(velocity_state, forcing_history, initial_velocity, viscosity, peclet_shaped, live_indicator, neighbour_holder, neighbour_slot)
    times = jnp.arange(WINDOW_SLICES, dtype=jnp.int32)
    product = (times[:, None] * times[None, :]) % WINDOW_SLICES
    angles = 2.0 * jnp.pi * product.astype(jnp.float32) / WINDOW_SLICES
    ramp = times.astype(jnp.float32) / WINDOW_SLICES
    twisted = jnp.power(ALPHA_SCALE, ramp)
    untwisted = jnp.power(ALPHA_SCALE, -ramp) / WINDOW_SLICES
    cosine = jnp.cos(angles)
    sine = jnp.sin(angles)
    source_real = jnp.einsum("kl,lncx->kncx", cosine * twisted[None, :], residual_value, precision=HIGHEST_PRECISION)
    source_imag = jnp.einsum("kl,lncx->kncx", -sine * twisted[None, :], residual_value, precision=HIGHEST_PRECISION)
    root = ALPHA_SCALE ** (1.0 / WINDOW_SLICES)
    base_angle = 2.0 * jnp.pi * times.astype(jnp.float32) / WINDOW_SLICES
    shift_real = (1.0 - root * jnp.cos(base_angle)) / STEP_DURATION
    shift_imag = root * jnp.sin(base_angle) / STEP_DURATION
    solver = partial(solve_frequency, viscosity=viscosity, peclet_shaped=peclet_shaped, neighbour_holder=neighbour_holder, neighbour_slot=neighbour_slot)
    real_component, imaginary_component = lax.map(solver, (source_real, source_imag, shift_real, shift_imag))
    update = jnp.einsum("lk,kncx->lncx", cosine * untwisted[:, None], real_component, precision=HIGHEST_PRECISION)
    update = update + jnp.einsum("lk,kncx->lncx", -sine * untwisted[:, None], imaginary_component, precision=HIGHEST_PRECISION)
    advanced_state = velocity_state + update
    corrected_residual = residual_grid(advanced_state, forcing_history, initial_velocity, viscosity, peclet_shaped, live_indicator, neighbour_holder, neighbour_slot)
    return jnp.transpose(advanced_state, (1, 0, 2, 3)), jnp.transpose(corrected_residual, (1, 0, 2, 3))
```

```python
import functools

import jax
import jax.numpy as jnp
from jax import lax
from jax.experimental import pallas as pl
from jax.experimental.pallas import tpu as pltpu
from jax.sharding import PartitionSpec as P

BLOCK_EDGE = 16
SWEEPS = 5
ALPHA_SCALE = 0.1

ROWS = 32
LANES = 128
COMPONENTS = 3
PLANES = BLOCK_EDGE
CELLS = PLANES * 8
TALL = CELLS + 24
WIDE = CELLS + 8
UNROLL = 4


def kernel(
    dims,
    holder,
    live,
    iterate,
    forcing,
    initial,
    viscosity,
    peclet,
    out_velocity,
    out_residual,
    stage_iterate,
    stage_forcing,
    field,
    local_field,
    source,
    force,
    start,
    ghost_y,
    ghost_z,
    coefficient,
    power,
    scale,
    gain,
    offset,
    carry_in,
    present,
    x_send,
    x_recv,
    y_send,
    y_recv,
    z_send,
    z_recv,
    x_end,
    y_end,
    z_end,
    end_recv,
    x_gain,
    y_gain,
    z_gain,
    x_offset,
    y_offset,
    z_offset,
    x_old,
    y_old,
    z_old,
    send_sem,
    recv_sem,
    stage_send,
    stage_recv,
    stage_local,
):
    chips, levels, slots, local = dims
    half = slots // 2
    times = 2 * local
    per_block = 2 * half
    me = lax.axis_index("tm")
    place = lax.axis_index("space")
    chip, core = me // 2, me % 2
    power_message = COMPONENTS * (SWEEPS + 1)

    sub = lax.broadcasted_iota(jnp.int32, (8, LANES), 0)
    lane = lax.broadcasted_iota(jnp.int32, (8, LANES), 1)
    z_index = lane % BLOCK_EDGE
    y_block = lane // BLOCK_EDGE
    y_upper = sub // half == 1
    slot_index = sub % half
    second = slot_index // 2 == 1
    first_block, last_block = y_block == 0, y_block == 7
    z_first, z_last = z_index == 0, z_index == BLOCK_EDGE - 1
    low_inner = (~y_upper) & second
    high_inner = y_upper & (~second)
    flat_lane = lax.broadcasted_iota(jnp.int32, (times, LANES), 1) // BLOCK_EDGE

    place_bit = [place // (1 << b) % 2 for b in range(levels)]

    def links_of(dim):
        found = []
        if dim < levels:
            side = 1 - place_bit[dim]
            if dim + 3 < levels:
                side = 1 - (place_bit[dim] + place_bit[dim + 3]) % 2
            found.append((side, place + (1 << dim) * (1 - 2 * place_bit[dim])))
            if dim + 3 < levels:
                far = dim + 3
                found.append((1 - side, place + (1 << far) * (1 - 2 * place_bit[far])))
        return found

    x_links, y_links, z_links = links_of(0), links_of(1), links_of(2)

    def seat(jump, which):
        return lax.rem(chip + jump, chips) * 2 + which

    greet = [{"tm": seat(j, core)} for j in range(1, chips)]
    for side, partner in x_links + y_links:
        greet += [{"space": partner, "tm": seat(j, core)} for j in range(chips)]
    greet += [{"tm": seat(j, 1 - core)} for j in range(chips)]
    for side, partner in z_links:
        greet += [{"space": partner, "tm": seat(j, 1 - core)} for j in range(chips)]
    barrier = pltpu.get_barrier_semaphore()
    for target in greet:
        pl.semaphore_signal(barrier, inc=1, device_id=target, device_id_type=pl.DeviceIdType.MESH)
    pl.semaphore_wait(barrier, len(greet))

    def remote(src, dst, sems, number, device):
        return pltpu.make_async_remote_copy(
            src_ref=src,
            dst_ref=dst,
            send_sem=sems[0].at[number],
            recv_sem=sems[1].at[number],
            device_id=device,
            device_id_type=pl.DeviceIdType.MESH,
        )

    peer = {"tm": seat(0, 1 - core)}
    mine = pl.ds(core * half, half)
    theirs = pl.ds((1 - core) * half, half)
    stage = (stage_send, stage_recv)
    swaps, owns = [], []
    for c in range(COMPONENTS):
        swaps.append(
            remote(iterate.at[theirs, c], stage_iterate.at[core, :, c], stage, c, peer)
        )
        owns.append(
            pltpu.make_async_copy(
                iterate.at[mine, c], stage_iterate.at[core, :, c], stage_local.at[c]
            )
        )
    for c in range(COMPONENTS):
        swaps.append(
            remote(forcing.at[theirs, c], stage_forcing.at[core, :, c], stage, COMPONENTS + c, peer)
        )
        owns.append(
            pltpu.make_async_copy(
                forcing.at[mine, c], stage_forcing.at[core, :, c], stage_local.at[COMPONENTS + c]
            )
        )
    for copy in swaps + owns:
        copy.start()

    per_message = (chips - 1) + chips * (len(x_links) + len(y_links) + 1 + len(z_links))

    def copies(message, buffer, pitch, base, c, carried=True):
        sems = (send_sem, recv_sem)
        number = [message * per_message]
        found = []

        def add(src, dst, device, condition=None):
            found.append((remote(src, dst, sems, number[0], device), condition))
            number[0] = number[0] + 1

        extra = range(1, chips) if carried else ()
        for n, (side, partner) in enumerate(x_links):
            add(x_send.at[message, n], x_recv.at[message, n], {"space": partner})
        for n, (side, partner) in enumerate(y_links):
            add(y_send.at[message, n], y_recv.at[message, n], {"space": partner})
        for side, partner in z_links:
            add(
                z_send.at[message, core],
                z_recv.at[message, 1 - core],
                {"space": partner, "tm": seat(0, 1 - core)},
                core == side,
            )
        add(z_send.at[message, 1 - core], z_recv.at[message, core], peer)
        for j in extra:
            last = pl.ds((times - 1) * pitch + base, CELLS)
            add(buffer.at[c, last], end_recv.at[message, j - 1], {"tm": seat(j, core)})
            for n, (side, partner) in enumerate(x_links):
                add(
                    x_send.at[message, n, pl.ds(times * 4, 8)],
                    x_end.at[message, n, j - 1],
                    {"space": partner, "tm": seat(j, core)},
                )
            for n, (side, partner) in enumerate(y_links):
                add(
                    y_send.at[message, n, pl.ds(32, 8)],
                    y_end.at[message, n, j - 1],
                    {"space": partner, "tm": seat(j, core)},
                )
            end = pl.ds((times - 1) * 8, 8)
            for side, partner in z_links:
                add(
                    z_send.at[message, core, end],
                    z_end.at[message, 1 - core, j - 1],
                    {"space": partner, "tm": seat(j, 1 - core)},
                    core == side,
                )
            add(
                z_send.at[message, 1 - core, end],
                z_end.at[message, core, j - 1],
                {"tm": seat(j, 1 - core)},
            )
        return found

    def start_all(found):
        for copy, condition in found:
            if condition is None:
                copy.start()
            else:
                pl.when(condition)(copy.start)

    def wait_all(found):
        for copy, condition in found:
            if condition is None:
                copy.wait()
            else:
                pl.when(condition)(copy.wait)

    outer_known = functools.reduce(
        jnp.logical_or, [core == side for side, partner in z_links], jnp.bool_(False)
    )

    def pack(message, load, pitch, base):
        for n, (side, partner) in enumerate(x_links):
            for t in range(times):
                value = load(pl.ds(t * pitch + base + side * (CELLS - 7), 4, stride=2))
                x_send[message, n, pl.ds(4 * t, 4), :] = value
            x_send[message, n, pl.ds(4 * times, 4), :] = value
            x_send[message, n, pl.ds(4 * times + 4, 4), :] = value
        for n, (side, partner) in enumerate(y_links):
            for k in range(4):
                total = None
                for i in range(8):
                    row = base + ((k % 2) * 8 + i) * 8 + k // 2 + side * 6
                    value = load(pl.ds(row, times, stride=pitch))
                    value = pltpu.roll(value, lax.rem(BLOCK_EDGE * i + 128 - 112 * side, 128), 1)
                    total = value if total is None else jnp.where(flat_lane == i, value, total)
                y_send[message, n, pl.ds(8 * k, times), :] = total
                y_send[message, n, pl.ds(32 + k, 1), :] = total[times - 1 : times]
                y_send[message, n, pl.ds(36 + k, 1), :] = total[times - 1 : times]
        for t in range(times):
            low = high = None
            for x in range(PLANES):
                value = load(pl.ds(t * pitch + base + 8 * x, 8))
                value = pltpu.roll(value, (x - 15) % 128, 1)
                high = value if high is None else jnp.where(z_index == x, value, high)
                low = value if low is None else jnp.where(z_index == (x + 1) % 16, value, low)
            z_send[message, 1, pl.ds(8 * t, 8), :] = high
            z_send[message, 0, pl.ds(8 * t, 8), :] = pltpu.roll(low, 15, 1)

    wraps = [jnp.where(chip - j < 0, ALPHA_SCALE, 1.0) for j in range(1, chips + 1)]
    keeps = [
        jnp.where(lax.rem(chip - j + chips, chips) == chips - 1, 0.0, 1.0)
        for j in range(1, chips + 1)
    ]

    def gains_of(ratio):
        powers = [jnp.ones_like(ratio)]
        for j in range(chips):
            powers.append(powers[-1] * ratio)
        scaled = 1.0 / (1.0 - ALPHA_SCALE * powers[chips])
        return [wraps[j] * (powers[j] * scaled) for j in range(chips)]

    def combine(gains, ends, weights=None):
        total = None
        for j in range(chips):
            term = gains[j] * ends[j]
            if weights is not None:
                term = term * weights[j]
            total = term if total is None else total + term
        return total

    def x_ends(message, n):
        found = [x_end[message, n, j, pl.ds(0, 4), :] for j in range(chips - 1)]
        return found + [x_recv[message, n, pl.ds(4 * times, 4), :]]

    def y_ends(message, n):
        found = [y_end[message, n, j, pl.ds(0, 4), :] for j in range(chips - 1)]
        return found + [y_recv[message, n, pl.ds(32, 4), :]]

    def z_ends(message, side):
        found = [z_end[message, side, j] for j in range(chips - 1)]
        return found + [z_recv[message, side, pl.ds(8 * (times - 1), 8), :]]

    def ghosts(message, c, mode):
        def finish(value, old, index):
            if mode == "raw":
                return value
            if mode == "last":
                return value - old[index]
            old[index] = value
            return value

        for t in range(times):
            base = t * TALL
            field[c, pl.ds(base, 8), :] = field[c, pl.ds(base + CELLS - 1, 8), :]
            field[c, pl.ds(base + CELLS + 8, 8), :] = field[c, pl.ds(base + 9, 8), :]
        for n, (side, partner) in enumerate(x_links):
            if mode == "raw":
                x_offset[c, n] = combine(
                    [x_gain[n, j] for j in range(chips)], x_ends(message, n), keeps
                )
            else:
                added = combine([x_gain[n, j] for j in range(chips)], x_ends(message, n))
                added = added + x_offset[c, n]
            for t in range(times):
                at = pl.ds(4 * t, 4)
                value = x_recv[message, n, at, :]
                if mode != "raw":
                    value = value + x_recv[power_message, n, at, :] * added
                value = finish(value, x_old, (c, n, at, slice(None)))
                field[c, pl.ds(t * TALL + side * (CELLS + 9), 4, stride=2), :] = value
        for n, (side, partner) in enumerate(y_links):
            if mode == "raw":
                y_offset[c, n] = combine(
                    [y_gain[n, j] for j in range(chips)], y_ends(message, n), keeps
                )
            else:
                added = combine([y_gain[n, j] for j in range(chips)], y_ends(message, n))
                added = added + y_offset[c, n]
            for k in range(4):
                at = pl.ds(8 * k, times)
                value = y_recv[message, n, at, :]
                if mode != "raw":
                    value = value + y_recv[power_message, n, at, :] * added[k : k + 1]
                value = finish(value, y_old, (c, n, at, slice(None)))
                for i in range(8):
                    turned = pltpu.roll(
                        value, lax.rem(112 * (1 - side) + 128 - BLOCK_EDGE * i, 128), 1
                    )
                    row = ((k % 2) * 8 + i) * 8 + k // 2 + side * 6
                    ghost_y[c, pl.ds(row, times, stride=WIDE), :] = turned
        added = [None, None]
        for side in range(2):
            ends = z_ends(message, side)
            gains = [z_gain[side, j] for j in range(chips)]
            if mode == "raw":
                z_offset[c, side] = combine(gains, ends, keeps)
            else:
                added[side] = combine(gains, ends) + z_offset[c, side]
        even = z_index % 2 == 0
        for t in range(times):
            at = pl.ds(8 * t, 8)
            pair = []
            for side in range(2):
                value = z_recv[message, side, at, :]
                if mode != "raw":
                    value = value + z_recv[power_message, side, at, :] * added[side]
                value = jnp.where((core != side) | outer_known, value, 0.0)
                pair.append(finish(value, z_old, (c, side, at, slice(None))))
            low, high = pair[0], pltpu.roll(pair[1], 15, 1)
            ghost_z[c, pl.ds(16 * t, 8), :] = jnp.where(even, low, high)
            ghost_z[c, pl.ds(16 * t + 8, 8), :] = jnp.where(even, high, low)

    def stencil(c, t, x, row, parity, factors):
        base = t * TALL + 8 + row

        def load(shift):
            return field[c, pl.ds(base + shift, 8), :]

        value = load(0)
        total = factors[0] * load(-8) + factors[1] * load(8)
        beyond = ghost_y[c, pl.ds(t * WIDE + row, 8), :]
        low = jnp.where(y_upper, load(-4), jnp.where(low_inner, load(2), beyond))
        low = pltpu.roll(jnp.where(last_block, low, value), 16, 1)
        high = jnp.where(y_upper, jnp.where(high_inner, load(-2), beyond), load(4))
        high = pltpu.roll(jnp.where(first_block, high, value), 112, 1)
        total = total + factors[2] * low + factors[3] * high
        edge = ghost_z[c, pl.ds(16 * t + 8 * parity, 8), :]
        edge = pltpu.roll(edge, lax.rem(128 - x, 128), 1)
        low = jnp.where(z_first, edge, pltpu.roll(value, 1, 1))
        high = jnp.where(z_last, edge, pltpu.roll(value, 127, 1))
        return value, total + factors[4] * low + factors[5] * high

    def over_planes(body):
        def one(group, carry):
            for i in range(UNROLL):
                x = group * UNROLL + i
                body(x, pl.multiple_of(x * 8, 8), i % 2)
            return carry

        lax.fori_loop(0, PLANES // UNROLL, one, 0)

    def factors_at(row):
        return [coefficient[f, pl.ds(row, 8), :] for f in range(6)]

    def sweep(c):
        def plane(x, row, parity):
            factors = factors_at(row)
            ratio = power[pl.ds(row, 8), :]
            before = None
            for t in range(times):
                _, total = stencil(c, t, x, row, parity, factors)
                total = total + source[c, pl.ds(t * CELLS + row, 8), :]
                if before is not None:
                    total = total + ratio * before
                local_field[c, pl.ds(t * WIDE + row, 8), :] = total
                before = total

        over_planes(plane)

    def first_residual(c):
        def plane(x, row, parity):
            factors = factors_at(row)
            ratio = power[pl.ds(row, 8), :]
            inverse = scale[pl.ds(row, 8), :]
            alive = present[6]
            earlier = jnp.where(chip == 0, start[c, pl.ds(row, 8), :], 0.0)
            before = None
            for t in range(times):
                value, total = stencil(c, t, x, row, parity, factors)
                total = total + inverse * force[c, pl.ds(t * CELLS + row, 8), :]
                total = (total + (ratio * earlier - value)) * alive
                source[c, pl.ds(t * CELLS + row, 8), :] = total
                if before is not None:
                    total = total + ratio * before
                local_field[c, pl.ds(t * WIDE + row, 8), :] = total
                before, earlier = total, value

        over_planes(plane)

    def own_ends(message, c, row):
        found = [end_recv[message, j, pl.ds(row, 8), :] for j in range(chips - 1)]
        return found

    def first_offset(message, c):
        def plane(x, row, parity):
            ends = own_ends(message, c, row)
            ends.append(field[c, pl.ds((times - 1) * TALL + 8 + row, 8), :])
            gains = [gain[j, pl.ds(row, 8), :] for j in range(chips)]
            offset[c, pl.ds(row, 8), :] = combine(gains, ends, keeps) * present[6]

        over_planes(plane)

    def complete(message, c, last):
        def plane(x, row, parity):
            ends = own_ends(message, c, row)
            ends.append(local_field[c, pl.ds((times - 1) * WIDE + row, 8), :])
            gains = [gain[j, pl.ds(row, 8), :] for j in range(chips)]
            added = combine(gains, ends) + offset[c, pl.ds(row, 8), :]
            if last:
                carry_in[c, pl.ds(row, 8), :] = added
            for t in range(times):
                value = local_field[c, pl.ds(t * WIDE + row, 8), :]
                value = value + power[pl.ds(t * WIDE + row, 8), :] * added
                at = pl.ds(t * TALL + 8 + row, 8)
                if last:
                    local_field[c, pl.ds(t * WIDE + row, 8), :] = value
                    value = value - field[c, at, :]
                field[c, at, :] = value

        over_planes(plane)

    def last_residual(c):
        def plane(x, row, parity):
            factors = factors_at(row)
            diagonal = 1.0 / scale[pl.ds(row, 8), :]
            for t in range(times):
                _, total = stencil(c, t, x, row, parity, factors)
                total = total * diagonal
                if t == 0:
                    added = carry_in[c, pl.ds(row, 8), :]
                    total = total - jnp.where(chip == 0, 2.0 * added, 0.0)
                source[c, pl.ds(t * CELLS + row, 8), :] = total

        over_planes(plane)

    def scatter(value, target, q):
        target[pl.ds(q, ROWS, stride=half), :] = value

    for q in range(half):
        slot = core * half + q
        scatter(viscosity[:, slot, :], scale, q)
        for d in range(3):
            scatter(peclet[d, :, slot, :], coefficient.at[2 * d], q)
        for c in range(COMPONENTS):
            scatter(initial[c, :, slot, :], start.at[c], q)
    for f in range(7):
        value = jnp.zeros((8, LANES), jnp.float32)
        for q in range(half):
            slot = core * half + q
            known = live[slot] > 0 if f == 6 else holder[slot, f] >= 0
            value = jnp.where(slot_index == q, jnp.where(known, 1.0, 0.0), value)
        present[f] = value

    def make(x, row, parity):
        at = pl.ds(row, 8)
        thickness = scale[at, :]
        inverse = 1.0 / (2.0 + 6.0 * thickness)
        scale[at, :] = inverse
        weight = thickness * inverse
        edges = [
            x == 0,
            x == PLANES - 1,
            (~y_upper) & first_block,
            y_upper & last_block,
            z_first,
            z_last,
        ]
        for d in range(3):
            number = coefficient[2 * d, at, :]
            for f, factor in ((2 * d, 1.0 + number), (2 * d + 1, 1.0 - number)):
                slot_edge = edges[f]
                value = weight * factor
                coefficient[f, at, :] = jnp.where(slot_edge, value * present[f], value)
        ratio = 2.0 * inverse
        total = ratio
        for t in range(times):
            power[pl.ds(t * WIDE + row, 8), :] = total
            if t == times - 1:
                for j, value in enumerate(gains_of(total)):
                    gain[j, at, :] = value
            total = total * ratio

    over_planes(make)
    ghost_y[...] = jnp.zeros_like(ghost_y)

    pack(power_message, lambda at: power[at, :], WIDE, 0)
    power_copies = copies(power_message, local_field, WIDE, 0, 0, carried=False)
    start_all(power_copies)

    def take(stage_ref, store):
        for origin in range(2):
            for j in range(local):
                for q in range(half):
                    store(origin * local + j, q, stage_ref[origin, q, :, j, :])

    for c in range(COMPONENTS):
        owns[c].wait()
        swaps[c].wait()

        def store(t, q, value, c=c):
            field[c, pl.ds(t * TALL + 8 + q, ROWS, stride=half), :] = value

        take(stage_iterate.at[:, :, c], store)
        pack(c, lambda at, c=c: field[c, at, :], TALL, 8)
        start_all(copies(c, field, TALL, 8, c))
    for c in range(COMPONENTS):
        owns[COMPONENTS + c].wait()
        swaps[COMPONENTS + c].wait()

        def store(t, q, value, c=c):
            force[c, pl.ds(t * CELLS + q, ROWS, stride=half), :] = value

        take(stage_forcing.at[:, :, c], store)

    wait_all(power_copies)
    for n in range(len(x_links)):
        for j, value in enumerate(gains_of(x_recv[power_message, n, pl.ds(4 * times, 4), :])):
            x_gain[n, j] = value
    for n in range(len(y_links)):
        for j, value in enumerate(gains_of(y_recv[power_message, n, pl.ds(32, 4), :])):
            y_gain[n, j] = value
    for side in range(2):
        ratio = z_recv[power_message, side, pl.ds(8 * (times - 1), 8), :]
        for j, value in enumerate(gains_of(ratio)):
            z_gain[side, j] = value

    def send_local(message, c):
        pack(message, lambda at: local_field[c, at, :], WIDE, 0)
        start_all(copies(message, local_field, WIDE, 0, c))

    def opening(c, carry):
        wait_all(copies(c, field, TALL, 8, c))
        ghosts(c, c, "raw")
        first_residual(c)
        send_local(COMPONENTS + c, c)
        first_offset(c, c)
        return carry

    lax.fori_loop(0, COMPONENTS, opening, 0)

    def turn(step, carry):
        c = lax.rem(step, COMPONENTS)
        message = COMPONENTS + step
        wait_all(copies(message, local_field, WIDE, 0, c))
        complete(message, c, False)
        ghosts(message, c, "next")
        sweep(c)
        send_local(message + COMPONENTS, c)
        return carry

    lax.fori_loop(0, COMPONENTS * (SWEEPS - 1), turn, 0)

    finals = []

    def give(c, stage_ref, load, out, number):
        for origin in range(2):
            for j in range(local):
                for q in range(half):
                    value = load(origin * local + j, q)
                    stage_ref[origin, q, c, :, j, :] = value(stage_ref[origin, q, c, :, j, :])
        other = 1 - core
        away = remote(
            stage_ref.at[other, :, c], out.at[mine, c], stage, number, peer
        )
        here = pltpu.make_async_copy(
            stage_ref.at[core, :, c], out.at[mine, c], stage_local.at[number]
        )
        away.start()
        here.start()
        finals.extend([away, here])

    for c in range(COMPONENTS):
        message = COMPONENTS * SWEEPS + c
        wait_all(copies(message, local_field, WIDE, 0, c))
        complete(message, c, True)

        def velocity(t, q, c=c):
            at = pl.ds(t * WIDE + q, ROWS, stride=half)
            return lambda held: held + local_field[c, at, :]

        give(c, stage_iterate, velocity, out_velocity, 2 * COMPONENTS + c)
        ghosts(message, c, "last")
        last_residual(c)

        def remainder(t, q, c=c):
            at = pl.ds(t * CELLS + q, ROWS, stride=half)
            return lambda held: source[c, at, :]

        give(c, stage_forcing, remainder, out_residual, 3 * COMPONENTS + c)
    for copy in finals:
        copy.wait()


def body(
    iterate,
    forcing,
    initial_velocity,
    viscosity,
    peclet,
    live_patch_mask,
    neighbour_holder,
    neighbour_slot,
):
    time_devices = lax.axis_size("tm")
    chips = time_devices // 2
    levels = lax.axis_size("space").bit_length() - 1
    slots, local = iterate.shape[:2]
    half = slots // 2
    times = 2 * local

    def by_rows(array):
        split = array.reshape(array.shape[:-1] + (ROWS, LANES))
        return split.transpose((0, 2, 3, 1, 4) if split.ndim == 5 else (1, 2, 0, 3))

    def whole(array):
        return array.transpose(0, 3, 1, 2, 4).reshape(slots, local, COMPONENTS, ROWS * LANES)

    count = [len(range(d, levels, 3)) for d in range(3)]
    messages = COMPONENTS * (SWEEPS + 1) + 1
    per_message = (chips - 1) + chips * (count[0] + count[1] + 1 + count[2])
    others = max(chips - 1, 1)
    f32 = jnp.float32
    stage = pltpu.VMEM((2, half, COMPONENTS, ROWS, local, LANES), f32)

    def rows(*shape):
        return pltpu.VMEM(shape + (LANES,), f32)

    nx, ny = max(count[0], 1), max(count[1], 1)
    x_rows, y_rows, z_rows = 4 * times + 8, 40, 8 * times
    result = jax.ShapeDtypeStruct((slots, COMPONENTS, ROWS, local, LANES), f32)
    velocity, residual = pl.pallas_call(
        functools.partial(kernel, (chips, levels, slots, local)),
        out_shape=(result, result),
        in_specs=[pl.BlockSpec(memory_space=pltpu.SMEM)] * 2
        + [pl.BlockSpec(memory_space=pl.ANY)] * 2
        + [pl.BlockSpec(memory_space=pltpu.VMEM)] * 3,
        out_specs=[pl.BlockSpec(memory_space=pl.ANY)] * 2,
        scratch_shapes=[
            stage,
            stage,
            rows(COMPONENTS, times * TALL),
            rows(COMPONENTS, times * WIDE),
            rows(COMPONENTS, times * CELLS),
            rows(COMPONENTS, times * CELLS),
            rows(COMPONENTS, CELLS),
            rows(COMPONENTS, times * WIDE),
            rows(COMPONENTS, times * 16),
            rows(6, CELLS),
            rows(times * WIDE),
            rows(CELLS),
            rows(chips, CELLS),
            rows(COMPONENTS, CELLS),
            rows(COMPONENTS, CELLS),
            rows(7, 8),
            rows(messages, nx, x_rows),
            rows(messages, nx, x_rows),
            rows(messages, ny, y_rows),
            rows(messages, ny, y_rows),
            rows(messages, 2, z_rows),
            rows(messages, 2, z_rows),
            rows(messages, nx, others, 8),
            rows(messages, ny, others, 8),
            rows(messages, 2, others, 8),
            rows(messages, others, CELLS),
            rows(nx, chips, 4),
            rows(ny, chips, 4),
            rows(2, chips, 8),
            rows(COMPONENTS, nx, 4),
            rows(COMPONENTS, ny, 4),
            rows(COMPONENTS, 2, 8),
            rows(COMPONENTS, nx, x_rows),
            rows(COMPONENTS, ny, y_rows),
            rows(COMPONENTS, 2, z_rows),
            pltpu.SemaphoreType.DMA((messages * per_message,)),
            pltpu.SemaphoreType.DMA((messages * per_message,)),
            pltpu.SemaphoreType.DMA((4 * COMPONENTS,)),
            pltpu.SemaphoreType.DMA((4 * COMPONENTS,)),
            pltpu.SemaphoreType.DMA((4 * COMPONENTS,)),
        ],
        compiler_params=pltpu.CompilerParams(
            collective_id=0, has_side_effects=True, vmem_limit_bytes=56 * 1024 * 1024
        ),
    )(
        neighbour_holder,
        live_patch_mask,
        by_rows(iterate),
        by_rows(forcing),
        by_rows(initial_velocity),
        viscosity.reshape(slots, ROWS, LANES).transpose(1, 0, 2),
        by_rows(peclet),
    )
    return whole(velocity), whole(residual)


def solution(mesh):
    return jax.shard_map(
        body,
        mesh=mesh,
        in_specs=(
            P("space", "tm", None, None),
            P("space", "tm", None, None),
            P("space", None, None),
            P("space", None),
            P("space", None, None),
            P("space"),
            P("space", None),
            P("space", None),
        ),
        out_specs=(P("space", "tm", None, None), P("space", "tm", None, None)),
        check_vma=False,
    )
```

```python
import functools

import jax
import jax.numpy as jnp
from jax import lax
from jax.experimental import pallas as pl
from jax.experimental.pallas import tpu as pltpu
from jax.sharding import PartitionSpec as P

BLOCK_EDGE = 16
SWEEPS = 5
ALPHA_SCALE = 0.1

ROWS = 32
LANES = 128
COMPONENTS = 3
PLANES = BLOCK_EDGE
CELLS = PLANES * 8
TALL = CELLS + 24
WIDE = CELLS + 8
UNROLL = 8


def kernel(
    dims,
    holder,
    live,
    iterate,
    forcing,
    initial,
    viscosity,
    peclet,
    out_velocity,
    out_residual,
    stage_iterate,
    stage_forcing,
    field,
    local_field,
    source,
    force,
    start,
    small_initial,
    small_viscosity,
    small_peclet,
    ghost_y,
    ghost_z,
    coefficient,
    power,
    scale,
    gain,
    end_send,
    carry,
    carry_in,
    present,
    x_send,
    x_recv,
    y_send,
    y_recv,
    z_send,
    z_recv,
    x_last,
    y_last,
    x_end,
    y_end,
    z_end,
    end_recv,
    x_gain,
    y_gain,
    z_gain,
    x_old,
    y_old,
    z_old,
    send_sem,
    recv_sem,
    stage_send,
    stage_recv,
    stage_local,
    small_sem,
):
    chips, levels, slots, local = dims
    half = slots // 2
    times = 2 * local
    per_block = 2 * half
    me = lax.axis_index("tm")
    place = lax.axis_index("space")
    chip, core = me // 2, me % 2
    power_message = COMPONENTS * (SWEEPS + 1)

    sub = lax.broadcasted_iota(jnp.int32, (8, LANES), 0)
    lane = lax.broadcasted_iota(jnp.int32, (8, LANES), 1)
    z_index = lane % BLOCK_EDGE
    y_block = lane // BLOCK_EDGE
    y_upper = sub // half == 1
    slot_index = sub % half
    second = slot_index // 2 == 1
    first_block, last_block = y_block == 0, y_block == 7
    z_first, z_last = z_index == 0, z_index == BLOCK_EDGE - 1
    low_inner = (~y_upper) & second
    high_inner = y_upper & (~second)
    flat_lane = lax.broadcasted_iota(jnp.int32, (times, LANES), 1) // BLOCK_EDGE

    place_bit = [place // (1 << b) % 2 for b in range(levels)]

    def links_of(dim):
        found = []
        if dim < levels:
            side = 1 - place_bit[dim]
            if dim + 3 < levels:
                side = 1 - (place_bit[dim] + place_bit[dim + 3]) % 2
            found.append((side, place + (1 << dim) * (1 - 2 * place_bit[dim])))
            if dim + 3 < levels:
                far = dim + 3
                found.append((1 - side, place + (1 << far) * (1 - 2 * place_bit[far])))
        return found

    x_links, y_links, z_links = links_of(0), links_of(1), links_of(2)

    def seat(jump, which):
        return lax.rem(chip + jump, chips) * 2 + which

    greet = [{"tm": seat(j, core)} for j in range(1, chips)]
    for side, partner in x_links + y_links:
        greet += [{"space": partner, "tm": seat(j, core)} for j in range(chips)]
    greet += [{"tm": seat(j, 1 - core)} for j in range(chips)]
    for side, partner in z_links:
        greet += [{"space": partner, "tm": seat(j, 1 - core)} for j in range(chips)]
    barrier = pltpu.get_barrier_semaphore()
    for target in greet:
        pl.semaphore_signal(barrier, inc=1, device_id=target, device_id_type=pl.DeviceIdType.MESH)
    smalls = [
        pltpu.make_async_copy(viscosity, small_viscosity, small_sem.at[0]),
        pltpu.make_async_copy(peclet, small_peclet, small_sem.at[1]),
        pltpu.make_async_copy(initial, small_initial, small_sem.at[2]),
    ]
    for copy in smalls:
        copy.start()

    def remote(src, dst, sems, number, device):
        return pltpu.make_async_remote_copy(
            src_ref=src,
            dst_ref=dst,
            send_sem=sems[0].at[number],
            recv_sem=sems[1].at[number],
            device_id=device,
            device_id_type=pl.DeviceIdType.MESH,
        )

    peer = {"tm": seat(0, 1 - core)}
    mine = pl.ds(core * half, half)
    theirs = pl.ds((1 - core) * half, half)
    stage = (stage_send, stage_recv)
    swaps, owns = [], []
    for c in range(COMPONENTS):
        swaps.append(
            remote(iterate.at[theirs, c], stage_iterate.at[core, :, c], stage, c, peer)
        )
        owns.append(
            pltpu.make_async_copy(
                iterate.at[mine, c], stage_iterate.at[core, :, c], stage_local.at[c]
            )
        )
    for c in range(COMPONENTS):
        swaps.append(
            remote(forcing.at[theirs, c], stage_forcing.at[core, :, c], stage, COMPONENTS + c, peer)
        )
        owns.append(
            pltpu.make_async_copy(
                forcing.at[mine, c], stage_forcing.at[core, :, c], stage_local.at[COMPONENTS + c]
            )
        )
    for copy in owns:
        copy.start()
    pl.semaphore_wait(barrier, len(greet))
    for copy in swaps:
        copy.start()

    per_message = (chips - 1) + chips * (len(x_links) + len(y_links) + 1 + len(z_links))

    def copies(message, c, ends=True):
        sems = (send_sem, recv_sem)
        number = [message * per_message]
        found = []

        def add(src, dst, device, condition=None):
            found.append((remote(src, dst, sems, number[0], device), condition))
            number[0] = number[0] + 1

        last = pl.ds(8 * times, 8)
        for j in range(1, chips) if ends else ():
            for n, (side, partner) in enumerate(x_links):
                add(
                    x_last.at[message, n],
                    x_end.at[message, n, j - 1],
                    {"space": partner, "tm": seat(j, core)},
                )
            for n, (side, partner) in enumerate(y_links):
                add(
                    y_last.at[message, n],
                    y_end.at[message, n, j - 1],
                    {"space": partner, "tm": seat(j, core)},
                )
            for side, partner in z_links:
                add(
                    z_send.at[message, core, last],
                    z_end.at[message, 1 - core, j - 1],
                    {"space": partner, "tm": seat(j, 1 - core)},
                    core == side,
                )
            add(
                z_send.at[message, 1 - core, last],
                z_end.at[message, core, j - 1],
                {"tm": seat(j, 1 - core)},
            )
            add(end_send.at[c], end_recv.at[message, j - 1], {"tm": seat(j, core)})
        for n, (side, partner) in enumerate(x_links):
            add(x_send.at[message, n], x_recv.at[message, n], {"space": partner})
        for n, (side, partner) in enumerate(y_links):
            add(y_send.at[message, n], y_recv.at[message, n], {"space": partner})
        for side, partner in z_links:
            add(
                z_send.at[message, core],
                z_recv.at[message, 1 - core],
                {"space": partner, "tm": seat(0, 1 - core)},
                core == side,
            )
        add(z_send.at[message, 1 - core], z_recv.at[message, core], peer)
        return found

    def start_all(found):
        for copy, condition in found:
            if condition is None:
                copy.start()
            else:
                pl.when(condition)(copy.start)

    def wait_all(found):
        for copy, condition in found:
            if condition is None:
                copy.wait()
            else:
                pl.when(condition)(copy.wait)

    outer_known = functools.reduce(
        jnp.logical_or, [core == side for side, partner in z_links], jnp.bool_(False)
    )

    kept = jnp.where(chip == chips - 1, 0.0, 1.0)

    def pack(message, load, pitch, base, first=None):
        for n, (side, partner) in enumerate(x_links):
            for t in range(times):
                value = load(pl.ds(t * pitch + base + side * (CELLS - 7), 4, stride=2))
                x_send[message, n, pl.ds(4 * t, 4), :] = value
            if first is not None:
                value = value + kept * x_send[first, n, pl.ds(4 * (times - 1), 4), :]
            x_send[message, n, pl.ds(4 * times, 4), :] = value
            x_send[message, n, pl.ds(4 * times + 4, 4), :] = value
            x_last[message, n] = value
        for n, (side, partner) in enumerate(y_links):
            for k in range(4):
                total = None
                for i in range(8):
                    row = base + ((k % 2) * 8 + i) * 8 + k // 2 + side * 6
                    value = load(pl.ds(row, times, stride=pitch))
                    value = pltpu.roll(value, lax.rem(BLOCK_EDGE * i + 128 - 112 * side, 128), 1)
                    total = value if total is None else jnp.where(flat_lane == i, value, total)
                y_send[message, n, pl.ds(8 * k, times), :] = total
                ending = total[times - 1 : times]
                if first is not None:
                    ending = ending + kept * y_send[first, n, pl.ds(8 * k + times - 1, 1), :]
                y_send[message, n, pl.ds(32 + k, 1), :] = ending
                y_send[message, n, pl.ds(36 + k, 1), :] = ending
                y_last[message, n, pl.ds(k, 1), :] = ending
        for t in range(times):
            low = high = None
            for x in range(PLANES):
                value = load(pl.ds(t * pitch + base + 8 * x, 8))
                value = pltpu.roll(value, (x - 15) % 128, 1)
                high = value if high is None else jnp.where(z_index == x, value, high)
                low = value if low is None else jnp.where(z_index == (x + 1) % 16, value, low)
            pair = (pltpu.roll(low, 15, 1), high)
            for side in range(2):
                z_send[message, side, pl.ds(8 * t, 8), :] = pair[side]
                if t == times - 1:
                    value = pair[side]
                    if first is not None:
                        value = value + kept * z_send[first, side, pl.ds(8 * t, 8), :]
                    z_send[message, side, pl.ds(8 * times, 8), :] = value

    wraps = [jnp.where(chip - j < 0, ALPHA_SCALE, 1.0) for j in range(1, chips + 1)]
    def gains_of(ratio):
        powers = [jnp.ones_like(ratio)]
        for j in range(chips):
            powers.append(powers[-1] * ratio)
        scaled = 1.0 / (1.0 - ALPHA_SCALE * powers[chips])
        return [wraps[j] * (powers[j] * scaled) for j in range(chips)]

    def combine(gains, ends):
        total = gains[0] * ends[0]
        for j in range(1, chips):
            total = total + gains[j] * ends[j]
        return total

    def x_ends(message, n):
        found = [x_end[message, n, j] for j in range(chips - 1)]
        return found + [x_recv[message, n, pl.ds(4 * times, 4), :]]

    def y_ends(message, n):
        found = [y_end[message, n, j] for j in range(chips - 1)]
        return found + [y_recv[message, n, pl.ds(32, 4), :]]

    def z_ends(message, side):
        found = [z_end[message, side, j] for j in range(chips - 1)]
        return found + [z_recv[message, side, pl.ds(8 * times, 8), :]]

    def ghosts(message, c, mode):
        def finish(value, old, index):
            if mode == "raw":
                return value
            if mode == "last":
                return value - old[index]
            old[index] = value
            return value

        for t in range(times):
            base = t * TALL
            field[c, pl.ds(base, 8), :] = field[c, pl.ds(base + CELLS - 1, 8), :]
            field[c, pl.ds(base + CELLS + 8, 8), :] = field[c, pl.ds(base + 9, 8), :]
        for n, (side, partner) in enumerate(x_links):
            if mode != "raw":
                added = combine([x_gain[n, j] for j in range(chips)], x_ends(message, n))
            for t in range(times):
                at = pl.ds(4 * t, 4)
                value = x_recv[message, n, at, :]
                if mode != "raw":
                    value = value + x_recv[power_message, n, at, :] * added
                value = finish(value, x_old, (c, n, at, slice(None)))
                field[c, pl.ds(t * TALL + side * (CELLS + 9), 4, stride=2), :] = value
        for n, (side, partner) in enumerate(y_links):
            if mode != "raw":
                added = combine([y_gain[n, j] for j in range(chips)], y_ends(message, n))
            for k in range(4):
                at = pl.ds(8 * k, times)
                value = y_recv[message, n, at, :]
                if mode != "raw":
                    value = value + y_recv[power_message, n, at, :] * added[k : k + 1]
                value = finish(value, y_old, (c, n, at, slice(None)))
                for i in range(8):
                    turned = pltpu.roll(
                        value, lax.rem(112 * (1 - side) + 128 - BLOCK_EDGE * i, 128), 1
                    )
                    row = ((k % 2) * 8 + i) * 8 + k // 2 + side * 6
                    ghost_y[c, pl.ds(row, times, stride=WIDE), :] = turned
        added = [None, None]
        for side in range(2):
            if mode != "raw":
                gains = [z_gain[side, j] for j in range(chips)]
                added[side] = combine(gains, z_ends(message, side))
        even = z_index % 2 == 0
        for t in range(times):
            at = pl.ds(8 * t, 8)
            pair = []
            for side in range(2):
                value = z_recv[message, side, at, :]
                if mode != "raw":
                    value = value + z_recv[power_message, side, at, :] * added[side]
                value = jnp.where((core != side) | outer_known, value, 0.0)
                pair.append(finish(value, z_old, (c, side, at, slice(None))))
            low, high = pair[0], pltpu.roll(pair[1], 15, 1)
            ghost_z[c, pl.ds(16 * t, 8), :] = jnp.where(even, low, high)
            ghost_z[c, pl.ds(16 * t + 8, 8), :] = jnp.where(even, high, low)

    def stencil(c, t, x, row, parity, factors):
        base = t * TALL + 8 + row

        def load(shift):
            return field[c, pl.ds(base + shift, 8), :]

        value = load(0)
        total = factors[0] * load(-8) + factors[1] * load(8)
        beyond = ghost_y[c, pl.ds(t * WIDE + row, 8), :]
        low = jnp.where(y_upper, load(-4), jnp.where(low_inner, load(2), beyond))
        low = pltpu.roll(jnp.where(last_block, low, value), 16, 1)
        high = jnp.where(y_upper, jnp.where(high_inner, load(-2), beyond), load(4))
        high = pltpu.roll(jnp.where(first_block, high, value), 112, 1)
        total = total + factors[2] * low + factors[3] * high
        edge = ghost_z[c, pl.ds(16 * t + 8 * parity, 8), :]
        edge = pltpu.roll(edge, lax.rem(128 - x, 128), 1)
        low = jnp.where(z_first, edge, pltpu.roll(value, 1, 1))
        high = jnp.where(z_last, edge, pltpu.roll(value, 127, 1))
        return value, total + factors[4] * low + factors[5] * high

    def over_planes(body):
        def one(group, carry):
            for i in range(UNROLL):
                x = group * UNROLL + i
                body(x, pl.multiple_of(x * 8, 8), i % 2)
            return carry

        lax.fori_loop(0, PLANES // UNROLL, one, 0)

    def factors_at(row):
        return [coefficient[f, pl.ds(row, 8), :] for f in range(6)]

    def sweep(c):
        def plane(x, row, parity):
            factors = factors_at(row)
            ratio = power[pl.ds(row, 8), :]
            before = None
            for t in range(times):
                _, total = stencil(c, t, x, row, parity, factors)
                total = total + source[c, pl.ds(t * CELLS + row, 8), :]
                if before is not None:
                    total = total + ratio * before
                local_field[c, pl.ds(t * WIDE + row, 8), :] = total
                before = total
            end_send[c, pl.ds(row, 8), :] = before + carry[c, pl.ds(row, 8), :]

        over_planes(plane)

    def first_residual(c):
        def plane(x, row, parity):
            factors = factors_at(row)
            ratio = power[pl.ds(row, 8), :]
            inverse = scale[pl.ds(row, 8), :]
            alive = present[6]
            earlier = jnp.where(chip == 0, start[c, pl.ds(row, 8), :], 0.0)
            before = None
            for t in range(times):
                value, total = stencil(c, t, x, row, parity, factors)
                total = total + inverse * force[c, pl.ds(t * CELLS + row, 8), :]
                total = (total + (ratio * earlier - value)) * alive
                source[c, pl.ds(t * CELLS + row, 8), :] = total
                if before is not None:
                    total = total + ratio * before
                local_field[c, pl.ds(t * WIDE + row, 8), :] = total
                before, earlier = total, value
            kept_end = kept * (earlier * alive)
            carry[c, pl.ds(row, 8), :] = kept_end
            end_send[c, pl.ds(row, 8), :] = before + kept_end

        over_planes(plane)

    def complete(message, c, last):
        def plane(x, row, parity):
            ends = [end_recv[message, j, pl.ds(row, 8), :] for j in range(chips - 1)]
            ends.append(end_send[c, pl.ds(row, 8), :])
            gains = [gain[j, pl.ds(row, 8), :] for j in range(chips)]
            added = combine(gains, ends)
            if last:
                carry_in[c, pl.ds(row, 8), :] = added
            for t in range(times):
                value = local_field[c, pl.ds(t * WIDE + row, 8), :]
                value = value + power[pl.ds(t * WIDE + row, 8), :] * added
                at = pl.ds(t * TALL + 8 + row, 8)
                if last:
                    local_field[c, pl.ds(t * WIDE + row, 8), :] = value
                    value = value - field[c, at, :]
                field[c, at, :] = value

        over_planes(plane)

    def last_residual(c):
        def plane(x, row, parity):
            factors = factors_at(row)
            diagonal = 1.0 / scale[pl.ds(row, 8), :]
            for t in range(times):
                _, total = stencil(c, t, x, row, parity, factors)
                total = total * diagonal
                if t == 0:
                    added = carry_in[c, pl.ds(row, 8), :]
                    total = total - jnp.where(chip == 0, 2.0 * added, 0.0)
                source[c, pl.ds(t * CELLS + row, 8), :] = total

        over_planes(plane)

    def scatter(value, target, q):
        target[pl.ds(q, ROWS, stride=half), :] = value

    for copy in smalls:
        copy.wait()
    for q in range(half):
        slot = core * half + q
        scatter(small_viscosity[:, slot, :], scale, q)
        for d in range(3):
            scatter(small_peclet[d, :, slot, :], coefficient.at[2 * d], q)
        for c in range(COMPONENTS):
            scatter(small_initial[c, :, slot, :], start.at[c], q)
    for f in range(7):
        value = jnp.zeros((8, LANES), jnp.float32)
        for q in range(half):
            slot = core * half + q
            known = live[slot] > 0 if f == 6 else holder[slot, f] >= 0
            value = jnp.where(slot_index == q, jnp.where(known, 1.0, 0.0), value)
        present[f] = value

    def make(x, row, parity):
        at = pl.ds(row, 8)
        thickness = scale[at, :]
        inverse = 1.0 / (2.0 + 6.0 * thickness)
        scale[at, :] = inverse
        weight = thickness * inverse
        edges = [
            x == 0,
            x == PLANES - 1,
            (~y_upper) & first_block,
            y_upper & last_block,
            z_first,
            z_last,
        ]
        for d in range(3):
            number = coefficient[2 * d, at, :]
            for f, factor in ((2 * d, 1.0 + number), (2 * d + 1, 1.0 - number)):
                slot_edge = edges[f]
                value = weight * factor
                coefficient[f, at, :] = jnp.where(slot_edge, value * present[f], value)
        ratio = 2.0 * inverse
        total = ratio
        for t in range(times):
            power[pl.ds(t * WIDE + row, 8), :] = total
            if t == times - 1:
                for j, value in enumerate(gains_of(total)):
                    gain[j, at, :] = value
            total = total * ratio

    over_planes(make)
    ghost_y[...] = jnp.zeros_like(ghost_y)

    pack(power_message, lambda at: power[at, :], WIDE, 0)
    power_copies = copies(power_message, 0, ends=False)
    start_all(power_copies)

    def take(stage_ref, store):
        for origin in range(2):
            for j in range(local):
                for q in range(half):
                    store(origin * local + j, q, stage_ref[origin, q, pl.ds(j, ROWS, stride=local), :])

    for c in range(COMPONENTS):
        owns[c].wait()
        swaps[c].wait()

        def store(t, q, value, c=c):
            field[c, pl.ds(t * TALL + 8 + q, ROWS, stride=half), :] = value

        take(stage_iterate.at[:, :, c], store)
        pack(c, lambda at, c=c: field[c, at, :], TALL, 8)
        start_all(copies(c, c, ends=False))
    for c in range(COMPONENTS):
        owns[COMPONENTS + c].wait()
        swaps[COMPONENTS + c].wait()

        def store(t, q, value, c=c):
            force[c, pl.ds(t * CELLS + q, ROWS, stride=half), :] = value

        take(stage_forcing.at[:, :, c], store)

    wait_all(power_copies)
    for n in range(len(x_links)):
        for j, value in enumerate(gains_of(x_recv[power_message, n, pl.ds(4 * times, 4), :])):
            x_gain[n, j] = value
    for n in range(len(y_links)):
        for j, value in enumerate(gains_of(y_recv[power_message, n, pl.ds(32, 4), :])):
            y_gain[n, j] = value
    for side in range(2):
        ratio = z_recv[power_message, side, pl.ds(8 * times, 8), :]
        for j, value in enumerate(gains_of(ratio)):
            z_gain[side, j] = value

    def send_local(message, c):
        pack(message, lambda at: local_field[c, at, :], WIDE, 0, c)
        start_all(copies(message, c))

    def opening(c, carry):
        wait_all(copies(c, c, ends=False))
        ghosts(c, c, "raw")
        first_residual(c)
        send_local(COMPONENTS + c, c)
        return carry

    lax.fori_loop(0, COMPONENTS, opening, 0)

    def turn(step, carry):
        c = lax.rem(step, COMPONENTS)
        message = COMPONENTS + step
        wait_all(copies(message, c))
        complete(message, c, False)
        ghosts(message, c, "next")
        sweep(c)
        send_local(message + COMPONENTS, c)
        return carry

    lax.fori_loop(0, COMPONENTS * (SWEEPS - 1), turn, 0)

    finals = []

    def give(c, stage_ref, load, out, number):
        for origin in range(2):
            for j in range(local):
                for q in range(half):
                    value = load(origin * local + j, q)
                    at = pl.ds(j, ROWS, stride=local)
                    stage_ref[origin, q, c, at, :] = value(stage_ref[origin, q, c, at, :])
        other = 1 - core
        away = remote(
            stage_ref.at[other, :, c], out.at[mine, c], stage, number, peer
        )
        here = pltpu.make_async_copy(
            stage_ref.at[core, :, c], out.at[mine, c], stage_local.at[number]
        )
        away.start()
        here.start()
        finals.extend([away, here])

    for c in range(COMPONENTS):
        message = COMPONENTS * SWEEPS + c
        wait_all(copies(message, c))
        complete(message, c, True)

        def velocity(t, q, c=c):
            at = pl.ds(t * WIDE + q, ROWS, stride=half)
            return lambda held: held + local_field[c, at, :]

        give(c, stage_iterate, velocity, out_velocity, 2 * COMPONENTS + c)
        ghosts(message, c, "last")
        last_residual(c)

        def remainder(t, q, c=c):
            at = pl.ds(t * CELLS + q, ROWS, stride=half)
            return lambda held: source[c, at, :]

        give(c, stage_forcing, remainder, out_residual, 3 * COMPONENTS + c)
    for copy in finals:
        copy.wait()


def body(
    iterate,
    forcing,
    initial_velocity,
    viscosity,
    peclet,
    live_patch_mask,
    neighbour_holder,
    neighbour_slot,
):
    time_devices = lax.axis_size("tm")
    chips = time_devices // 2
    levels = lax.axis_size("space").bit_length() - 1
    slots, local = iterate.shape[:2]
    half = slots // 2
    times = 2 * local

    def by_rows(array):
        split = array.reshape(array.shape[:-1] + (ROWS, LANES))
        if split.ndim == 4:
            return split.transpose(1, 2, 0, 3)
        split = split.transpose(0, 2, 3, 1, 4)
        return split.reshape(slots, COMPONENTS, ROWS * local, LANES)

    def whole(array):
        split = array.reshape(slots, COMPONENTS, ROWS, local, LANES)
        return split.transpose(0, 3, 1, 2, 4).reshape(slots, local, COMPONENTS, ROWS * LANES)

    count = [len(range(d, levels, 3)) for d in range(3)]
    messages = COMPONENTS * (SWEEPS + 1) + 1
    per_message = (chips - 1) + chips * (count[0] + count[1] + 1 + count[2])
    others = max(chips - 1, 1)
    f32 = jnp.float32
    stage = pltpu.VMEM((2, half, COMPONENTS, ROWS * local, LANES), f32)

    def rows(*shape):
        return pltpu.VMEM(shape + (LANES,), f32)

    nx, ny = max(count[0], 1), max(count[1], 1)
    x_rows, y_rows, z_rows = 4 * times + 8, 40, 8 * times + 8
    result = jax.ShapeDtypeStruct((slots, COMPONENTS, ROWS * local, LANES), f32)
    velocity, residual = pl.pallas_call(
        functools.partial(kernel, (chips, levels, slots, local)),
        out_shape=(result, result),
        in_specs=[pl.BlockSpec(memory_space=pltpu.SMEM)] * 2
        + [pl.BlockSpec(memory_space=pl.ANY)] * 5,
        out_specs=[pl.BlockSpec(memory_space=pl.ANY)] * 2,
        scratch_shapes=[
            stage,
            stage,
            rows(COMPONENTS, times * TALL),
            rows(COMPONENTS, times * WIDE),
            rows(COMPONENTS, times * CELLS),
            rows(COMPONENTS, times * CELLS),
            rows(COMPONENTS, CELLS),
            rows(COMPONENTS, ROWS, slots),
            rows(ROWS, slots),
            rows(COMPONENTS, ROWS, slots),
            rows(COMPONENTS, times * WIDE),
            rows(COMPONENTS, times * 16),
            rows(6, CELLS),
            rows(times * WIDE),
            rows(CELLS),
            rows(chips, CELLS),
            rows(COMPONENTS, CELLS),
            rows(COMPONENTS, CELLS),
            rows(COMPONENTS, CELLS),
            rows(7, 8),
            rows(messages, nx, x_rows),
            rows(messages, nx, x_rows),
            rows(messages, ny, y_rows),
            rows(messages, ny, y_rows),
            rows(messages, 2, z_rows),
            rows(messages, 2, z_rows),
            rows(messages, nx, 4),
            rows(messages, ny, 4),
            rows(messages, nx, others, 4),
            rows(messages, ny, others, 4),
            rows(messages, 2, others, 8),
            rows(messages, others, CELLS),
            rows(nx, chips, 4),
            rows(ny, chips, 4),
            rows(2, chips, 8),
            rows(COMPONENTS, nx, x_rows),
            rows(COMPONENTS, ny, y_rows),
            rows(COMPONENTS, 2, z_rows),
            pltpu.SemaphoreType.DMA((messages * per_message,)),
            pltpu.SemaphoreType.DMA((messages * per_message,)),
            pltpu.SemaphoreType.DMA((4 * COMPONENTS,)),
            pltpu.SemaphoreType.DMA((4 * COMPONENTS,)),
            pltpu.SemaphoreType.DMA((4 * COMPONENTS,)),
            pltpu.SemaphoreType.DMA((3,)),
        ],
        compiler_params=pltpu.CompilerParams(
            collective_id=0, has_side_effects=True, vmem_limit_bytes=56 * 1024 * 1024
        ),
    )(
        neighbour_holder,
        live_patch_mask,
        by_rows(iterate),
        by_rows(forcing),
        by_rows(initial_velocity),
        viscosity.reshape(slots, ROWS, LANES).transpose(1, 0, 2),
        by_rows(peclet),
    )
    return whole(velocity), whole(residual)


def solution(mesh):
    return jax.shard_map(
        body,
        mesh=mesh,
        in_specs=(
            P("space", "tm", None, None),
            P("space", "tm", None, None),
            P("space", None, None),
            P("space", None),
            P("space", None, None),
            P("space"),
            P("space", None),
            P("space", None),
        ),
        out_specs=(P("space", "tm", None, None), P("space", "tm", None, None)),
        check_vma=False,
    )
```

```python
import functools

import jax
import jax.numpy as jnp
from jax import lax
from jax.experimental import pallas as pl
from jax.experimental.pallas import tpu as pltpu
from jax.sharding import PartitionSpec as P

BLOCK_EDGE = 16
SWEEPS = 5
ALPHA_SCALE = 0.1

ROWS = 32
LANES = 128
COMPONENTS = 3
PLANES = BLOCK_EDGE
CELLS = PLANES * 8
TALL = CELLS + 24
WIDE = CELLS + 8
UNROLL = 16


def kernel(
    dims,
    holder,
    live,
    iterate,
    forcing,
    initial,
    viscosity,
    peclet,
    out_velocity,
    out_residual,
    stage_iterate,
    stage_forcing,
    field,
    local_field,
    source,
    force,
    start,
    small_initial,
    small_viscosity,
    small_peclet,
    ghost_y,
    ghost_z,
    coefficient,
    power,
    scale,
    gain,
    end_send,
    carry,
    carry_in,
    present,
    x_send,
    x_recv,
    y_send,
    y_recv,
    z_send,
    z_recv,
    x_last,
    y_last,
    x_end,
    y_end,
    z_end,
    end_recv,
    x_gain,
    y_gain,
    z_gain,
    x_old,
    y_old,
    z_old,
    send_sem,
    recv_sem,
    stage_send,
    stage_recv,
    stage_local,
    small_sem,
):
    chips, levels, slots, local = dims
    half = slots // 2
    times = 2 * local
    per_block = 2 * half
    me = lax.axis_index("tm")
    place = lax.axis_index("space")
    chip, core = me // 2, me % 2
    power_message = COMPONENTS * (SWEEPS + 1)

    sub = lax.broadcasted_iota(jnp.int32, (8, LANES), 0)
    lane = lax.broadcasted_iota(jnp.int32, (8, LANES), 1)
    z_index = lane % BLOCK_EDGE
    y_block = lane // BLOCK_EDGE
    y_upper = sub // half == 1
    slot_index = sub % half
    second = slot_index // 2 == 1
    first_block, last_block = y_block == 0, y_block == 7
    z_first, z_last = z_index == 0, z_index == BLOCK_EDGE - 1
    low_inner = (~y_upper) & second
    high_inner = y_upper & (~second)
    flat_lane = lax.broadcasted_iota(jnp.int32, (times, LANES), 1) // BLOCK_EDGE

    place_bit = [place // (1 << b) % 2 for b in range(levels)]

    def links_of(dim):
        found = []
        if dim < levels:
            side = 1 - place_bit[dim]
            if dim + 3 < levels:
                side = 1 - (place_bit[dim] + place_bit[dim + 3]) % 2
            found.append((side, place + (1 << dim) * (1 - 2 * place_bit[dim])))
            if dim + 3 < levels:
                far = dim + 3
                found.append((1 - side, place + (1 << far) * (1 - 2 * place_bit[far])))
        return found

    x_links, y_links, z_links = links_of(0), links_of(1), links_of(2)

    def seat(jump, which):
        return lax.rem(chip + jump, chips) * 2 + which

    greet = [{"tm": seat(j, core)} for j in range(1, chips)]
    for side, partner in x_links + y_links:
        greet += [{"space": partner, "tm": seat(j, core)} for j in range(chips)]
    greet += [{"tm": seat(j, 1 - core)} for j in range(chips)]
    for side, partner in z_links:
        greet += [{"space": partner, "tm": seat(j, 1 - core)} for j in range(chips)]
    barrier = pltpu.get_barrier_semaphore()
    for target in greet:
        pl.semaphore_signal(barrier, inc=1, device_id=target, device_id_type=pl.DeviceIdType.MESH)
    smalls = [
        pltpu.make_async_copy(viscosity, small_viscosity, small_sem.at[0]),
        pltpu.make_async_copy(peclet, small_peclet, small_sem.at[1]),
        pltpu.make_async_copy(initial, small_initial, small_sem.at[2]),
    ]
    for copy in smalls:
        copy.start()

    def remote(src, dst, sems, number, device):
        return pltpu.make_async_remote_copy(
            src_ref=src,
            dst_ref=dst,
            send_sem=sems[0].at[number],
            recv_sem=sems[1].at[number],
            device_id=device,
            device_id_type=pl.DeviceIdType.MESH,
        )

    peer = {"tm": seat(0, 1 - core)}
    mine = pl.ds(core * half, half)
    theirs = pl.ds((1 - core) * half, half)
    stage = (stage_send, stage_recv)
    swaps, owns = [], []
    for c in range(COMPONENTS):
        swaps.append(
            remote(iterate.at[theirs, c], stage_iterate.at[core, :, c], stage, c, peer)
        )
        owns.append(
            pltpu.make_async_copy(
                iterate.at[mine, c], stage_iterate.at[core, :, c], stage_local.at[c]
            )
        )
    for c in range(COMPONENTS):
        swaps.append(
            remote(forcing.at[theirs, c], stage_forcing.at[core, :, c], stage, COMPONENTS + c, peer)
        )
        owns.append(
            pltpu.make_async_copy(
                forcing.at[mine, c], stage_forcing.at[core, :, c], stage_local.at[COMPONENTS + c]
            )
        )
    for copy in owns:
        copy.start()
    pl.semaphore_wait(barrier, len(greet))
    for copy in swaps:
        copy.start()

    per_message = (chips - 1) + chips * (len(x_links) + len(y_links) + 1 + len(z_links))

    def copies(message, ends=True):
        sems = (send_sem, recv_sem)
        number = [message * per_message]
        found = []

        def add(src, dst, device, condition=None):
            found.append((remote(src, dst, sems, number[0], device), condition))
            number[0] = number[0] + 1

        last = pl.ds(8 * times, 8)
        number[0] = number[0] + chips - 1
        for j in range(1, chips) if ends else ():
            for n, (side, partner) in enumerate(x_links):
                add(
                    x_last.at[message, n],
                    x_end.at[message, n, j - 1],
                    {"space": partner, "tm": seat(j, core)},
                )
            for n, (side, partner) in enumerate(y_links):
                add(
                    y_last.at[message, n],
                    y_end.at[message, n, j - 1],
                    {"space": partner, "tm": seat(j, core)},
                )
            for side, partner in z_links:
                add(
                    z_send.at[message, core, last],
                    z_end.at[message, 1 - core, j - 1],
                    {"space": partner, "tm": seat(j, 1 - core)},
                    core == side,
                )
            add(
                z_send.at[message, 1 - core, last],
                z_end.at[message, core, j - 1],
                {"tm": seat(j, 1 - core)},
            )
        for n, (side, partner) in enumerate(x_links):
            add(x_send.at[message, n], x_recv.at[message, n], {"space": partner})
        for n, (side, partner) in enumerate(y_links):
            add(y_send.at[message, n], y_recv.at[message, n], {"space": partner})
        for side, partner in z_links:
            add(
                z_send.at[message, core],
                z_recv.at[message, 1 - core],
                {"space": partner, "tm": seat(0, 1 - core)},
                core == side,
            )
        add(z_send.at[message, 1 - core], z_recv.at[message, core], peer)
        return found

    def carries(message, c):
        return [
            (
                remote(
                    end_send.at[c],
                    end_recv.at[message, j - 1],
                    (send_sem, recv_sem),
                    message * per_message + j - 1,
                    {"tm": seat(j, core)},
                ),
                None,
            )
            for j in range(1, chips)
        ]

    def start_all(found):
        for copy, condition in found:
            if condition is None:
                copy.start()
            else:
                pl.when(condition)(copy.start)

    def wait_all(found):
        for copy, condition in found:
            if condition is None:
                copy.wait()
            else:
                pl.when(condition)(copy.wait)

    outer_known = functools.reduce(
        jnp.logical_or, [core == side for side, partner in z_links], jnp.bool_(False)
    )

    kept = jnp.where(chip == chips - 1, 0.0, 1.0)

    def pack(message, load, pitch, base, first=None):
        for n, (side, partner) in enumerate(x_links):
            for t in range(times):
                value = load(pl.ds(t * pitch + base + side * (CELLS - 7), 4, stride=2))
                x_send[message, n, pl.ds(4 * t, 4), :] = value
            if first is not None:
                value = value + kept * x_send[first, n, pl.ds(4 * (times - 1), 4), :]
            x_send[message, n, pl.ds(4 * times, 4), :] = value
            x_send[message, n, pl.ds(4 * times + 4, 4), :] = value
            x_last[message, n] = value
        for n, (side, partner) in enumerate(y_links):
            for k in range(4):
                total = None
                for i in range(8):
                    row = base + ((k % 2) * 8 + i) * 8 + k // 2 + side * 6
                    value = load(pl.ds(row, times, stride=pitch))
                    value = pltpu.roll(value, lax.rem(BLOCK_EDGE * i + 128 - 112 * side, 128), 1)
                    total = value if total is None else jnp.where(flat_lane == i, value, total)
                y_send[message, n, pl.ds(8 * k, times), :] = total
                ending = total[times - 1 : times]
                if first is not None:
                    ending = ending + kept * y_send[first, n, pl.ds(8 * k + times - 1, 1), :]
                y_send[message, n, pl.ds(32 + k, 1), :] = ending
                y_send[message, n, pl.ds(36 + k, 1), :] = ending
                y_last[message, n, pl.ds(k, 1), :] = ending
        for t in range(times):
            low = high = None
            for x in range(PLANES):
                value = load(pl.ds(t * pitch + base + 8 * x, 8))
                value = pltpu.roll(value, (x - 15) % 128, 1)
                high = value if high is None else jnp.where(z_index == x, value, high)
                low = value if low is None else jnp.where(z_index == (x + 1) % 16, value, low)
            pair = (pltpu.roll(low, 15, 1), high)
            for side in range(2):
                z_send[message, side, pl.ds(8 * t, 8), :] = pair[side]
                if t == times - 1:
                    value = pair[side]
                    if first is not None:
                        value = value + kept * z_send[first, side, pl.ds(8 * t, 8), :]
                    z_send[message, side, pl.ds(8 * times, 8), :] = value

    wraps = [jnp.where(chip - j < 0, ALPHA_SCALE, 1.0) for j in range(1, chips + 1)]
    def gains_of(ratio):
        powers = [jnp.ones_like(ratio)]
        for j in range(chips):
            powers.append(powers[-1] * ratio)
        scaled = 1.0 / (1.0 - ALPHA_SCALE * powers[chips])
        return [wraps[j] * (powers[j] * scaled) for j in range(chips)]

    def combine(gains, ends):
        total = gains[0] * ends[0]
        for j in range(1, chips):
            total = total + gains[j] * ends[j]
        return total

    def x_ends(message, n):
        found = [x_end[message, n, j] for j in range(chips - 1)]
        return found + [x_recv[message, n, pl.ds(4 * times, 4), :]]

    def y_ends(message, n):
        found = [y_end[message, n, j] for j in range(chips - 1)]
        return found + [y_recv[message, n, pl.ds(32, 4), :]]

    def z_ends(message, side):
        found = [z_end[message, side, j] for j in range(chips - 1)]
        return found + [z_recv[message, side, pl.ds(8 * times, 8), :]]

    def ghosts(message, c, mode):
        def finish(value, old, index):
            if mode == "raw":
                return value
            if mode == "last":
                return value - old[index]
            old[index] = value
            return value

        for t in range(times):
            base = t * TALL
            field[c, pl.ds(base, 8), :] = field[c, pl.ds(base + CELLS - 1, 8), :]
            field[c, pl.ds(base + CELLS + 8, 8), :] = field[c, pl.ds(base + 9, 8), :]
        for n, (side, partner) in enumerate(x_links):
            if mode != "raw":
                added = combine([x_gain[n, j] for j in range(chips)], x_ends(message, n))
            for t in range(times):
                at = pl.ds(4 * t, 4)
                value = x_recv[message, n, at, :]
                if mode != "raw":
                    value = value + x_recv[power_message, n, at, :] * added
                value = finish(value, x_old, (c, n, at, slice(None)))
                field[c, pl.ds(t * TALL + side * (CELLS + 9), 4, stride=2), :] = value
        for n, (side, partner) in enumerate(y_links):
            if mode != "raw":
                added = combine([y_gain[n, j] for j in range(chips)], y_ends(message, n))
            for k in range(4):
                at = pl.ds(8 * k, times)
                value = y_recv[message, n, at, :]
                if mode != "raw":
                    value = value + y_recv[power_message, n, at, :] * added[k : k + 1]
                value = finish(value, y_old, (c, n, at, slice(None)))
                for i in range(8):
                    turned = pltpu.roll(
                        value, lax.rem(112 * (1 - side) + 128 - BLOCK_EDGE * i, 128), 1
                    )
                    row = ((k % 2) * 8 + i) * 8 + k // 2 + side * 6
                    ghost_y[c, pl.ds(row, times, stride=WIDE), :] = turned
        added = [None, None]
        for side in range(2):
            if mode != "raw":
                gains = [z_gain[side, j] for j in range(chips)]
                added[side] = combine(gains, z_ends(message, side))
        even = z_index % 2 == 0
        for t in range(times):
            at = pl.ds(8 * t, 8)
            pair = []
            for side in range(2):
                value = z_recv[message, side, at, :]
                if mode != "raw":
                    value = value + z_recv[power_message, side, at, :] * added[side]
                value = jnp.where((core != side) | outer_known, value, 0.0)
                pair.append(finish(value, z_old, (c, side, at, slice(None))))
            low, high = pair[0], pltpu.roll(pair[1], 15, 1)
            ghost_z[c, pl.ds(16 * t, 8), :] = jnp.where(even, low, high)
            ghost_z[c, pl.ds(16 * t + 8, 8), :] = jnp.where(even, high, low)

    def stencil(c, t, x, row, parity, factors):
        base = t * TALL + 8 + row

        def load(shift):
            return field[c, pl.ds(base + shift, 8), :]

        value = load(0)
        total = factors[0] * load(-8) + factors[1] * load(8)
        beyond = ghost_y[c, pl.ds(t * WIDE + row, 8), :]
        low = jnp.where(y_upper, load(-4), jnp.where(low_inner, load(2), beyond))
        low = pltpu.roll(jnp.where(last_block, low, value), 16, 1)
        high = jnp.where(y_upper, jnp.where(high_inner, load(-2), beyond), load(4))
        high = pltpu.roll(jnp.where(first_block, high, value), 112, 1)
        total = total + factors[2] * low + factors[3] * high
        edge = ghost_z[c, pl.ds(16 * t + 8 * parity, 8), :]
        edge = pltpu.roll(edge, lax.rem(128 - x, 128), 1)
        low = jnp.where(z_first, edge, pltpu.roll(value, 1, 1))
        high = jnp.where(z_last, edge, pltpu.roll(value, 127, 1))
        return value, total + factors[4] * low + factors[5] * high

    def over_planes(body):
        def one(group, carry):
            for i in range(UNROLL):
                x = group * UNROLL + i
                body(x, pl.multiple_of(x * 8, 8), i % 2)
            return carry

        lax.fori_loop(0, PLANES // UNROLL, one, 0)

    def factors_at(row):
        return [coefficient[f, pl.ds(row, 8), :] for f in range(6)]

    def sweep(c):
        def plane(x, row, parity):
            factors = factors_at(row)
            ratio = power[pl.ds(row, 8), :]
            before = None
            for t in range(times):
                _, total = stencil(c, t, x, row, parity, factors)
                total = total + source[c, pl.ds(t * CELLS + row, 8), :]
                if before is not None:
                    total = total + ratio * before
                local_field[c, pl.ds(t * WIDE + row, 8), :] = total
                before = total
            end_send[c, pl.ds(row, 8), :] = before + carry[c, pl.ds(row, 8), :]

        over_planes(plane)

    def first_residual(c):
        def plane(x, row, parity):
            factors = factors_at(row)
            ratio = power[pl.ds(row, 8), :]
            inverse = scale[pl.ds(row, 8), :]
            alive = present[6]
            earlier = jnp.where(chip == 0, start[c, pl.ds(row, 8), :], 0.0)
            before = None
            for t in range(times):
                value, total = stencil(c, t, x, row, parity, factors)
                total = total + inverse * force[c, pl.ds(t * CELLS + row, 8), :]
                total = (total + (ratio * earlier - value)) * alive
                source[c, pl.ds(t * CELLS + row, 8), :] = total
                if before is not None:
                    total = total + ratio * before
                local_field[c, pl.ds(t * WIDE + row, 8), :] = total
                before, earlier = total, value
            kept_end = kept * (earlier * alive)
            carry[c, pl.ds(row, 8), :] = kept_end
            end_send[c, pl.ds(row, 8), :] = before + kept_end

        over_planes(plane)

    def complete(message, c, last):
        def plane(x, row, parity):
            ends = [end_recv[message, j, pl.ds(row, 8), :] for j in range(chips - 1)]
            ends.append(end_send[c, pl.ds(row, 8), :])
            gains = [gain[j, pl.ds(row, 8), :] for j in range(chips)]
            added = combine(gains, ends)
            if last:
                carry_in[c, pl.ds(row, 8), :] = added
            for t in range(times):
                value = local_field[c, pl.ds(t * WIDE + row, 8), :]
                value = value + power[pl.ds(t * WIDE + row, 8), :] * added
                at = pl.ds(t * TALL + 8 + row, 8)
                if last:
                    local_field[c, pl.ds(t * WIDE + row, 8), :] = value
                    value = value - field[c, at, :]
                field[c, at, :] = value

        over_planes(plane)

    def last_residual(c):
        def plane(x, row, parity):
            factors = factors_at(row)
            diagonal = 1.0 / scale[pl.ds(row, 8), :]
            for t in range(times):
                _, total = stencil(c, t, x, row, parity, factors)
                total = total * diagonal
                if t == 0:
                    added = carry_in[c, pl.ds(row, 8), :]
                    total = total - jnp.where(chip == 0, 2.0 * added, 0.0)
                source[c, pl.ds(t * CELLS + row, 8), :] = total

        over_planes(plane)

    def scatter(value, target, q):
        target[pl.ds(q, ROWS, stride=half), :] = value

    for copy in smalls:
        copy.wait()
    for q in range(half):
        slot = core * half + q
        scatter(small_viscosity[:, slot, :], scale, q)
        for d in range(3):
            scatter(small_peclet[d, :, slot, :], coefficient.at[2 * d], q)
        for c in range(COMPONENTS):
            scatter(small_initial[c, :, slot, :], start.at[c], q)
    for f in range(7):
        value = jnp.zeros((8, LANES), jnp.float32)
        for q in range(half):
            slot = core * half + q
            known = live[slot] > 0 if f == 6 else holder[slot, f] >= 0
            value = jnp.where(slot_index == q, jnp.where(known, 1.0, 0.0), value)
        present[f] = value

    def make(x, row, parity):
        at = pl.ds(row, 8)
        thickness = scale[at, :]
        inverse = 1.0 / (2.0 + 6.0 * thickness)
        scale[at, :] = inverse
        weight = thickness * inverse
        edges = [
            x == 0,
            x == PLANES - 1,
            (~y_upper) & first_block,
            y_upper & last_block,
            z_first,
            z_last,
        ]
        for d in range(3):
            number = coefficient[2 * d, at, :]
            for f, factor in ((2 * d, 1.0 + number), (2 * d + 1, 1.0 - number)):
                slot_edge = edges[f]
                value = weight * factor
                coefficient[f, at, :] = jnp.where(slot_edge, value * present[f], value)
        ratio = 2.0 * inverse
        total = ratio
        for t in range(times):
            power[pl.ds(t * WIDE + row, 8), :] = total
            if t == times - 1:
                for j, value in enumerate(gains_of(total)):
                    gain[j, at, :] = value
            total = total * ratio

    over_planes(make)
    ghost_y[...] = jnp.zeros_like(ghost_y)

    pack(power_message, lambda at: power[at, :], WIDE, 0)
    power_copies = copies(power_message, ends=False)
    start_all(power_copies)

    def take(stage_ref, store):
        for origin in range(2):
            for j in range(local):
                for q in range(half):
                    store(origin * local + j, q, stage_ref[origin, q, pl.ds(j, ROWS, stride=local), :])

    for c in range(COMPONENTS):
        owns[c].wait()
        swaps[c].wait()

        def store(t, q, value, c=c):
            field[c, pl.ds(t * TALL + 8 + q, ROWS, stride=half), :] = value

        take(stage_iterate.at[:, :, c], store)
        pack(c, lambda at, c=c: field[c, at, :], TALL, 8)
        start_all(copies(c, ends=False))
    for c in range(COMPONENTS):
        owns[COMPONENTS + c].wait()
        swaps[COMPONENTS + c].wait()

        def store(t, q, value, c=c):
            force[c, pl.ds(t * CELLS + q, ROWS, stride=half), :] = value

        take(stage_forcing.at[:, :, c], store)

    wait_all(power_copies)
    for n in range(len(x_links)):
        for j, value in enumerate(gains_of(x_recv[power_message, n, pl.ds(4 * times, 4), :])):
            x_gain[n, j] = value
    for n in range(len(y_links)):
        for j, value in enumerate(gains_of(y_recv[power_message, n, pl.ds(32, 4), :])):
            y_gain[n, j] = value
    for side in range(2):
        ratio = z_recv[power_message, side, pl.ds(8 * times, 8), :]
        for j, value in enumerate(gains_of(ratio)):
            z_gain[side, j] = value

    def send_local(message, c):
        pack(message, lambda at: local_field[c, at, :], WIDE, 0, c)
        start_all(copies(message))
        start_all(carries(message, c))

    def opening(c, carry):
        wait_all(copies(c, ends=False))
        ghosts(c, c, "raw")
        first_residual(c)
        send_local(COMPONENTS + c, c)
        return carry

    lax.fori_loop(0, COMPONENTS, opening, 0)

    def turn(step, carry):
        c = lax.rem(step, COMPONENTS)
        message = COMPONENTS + step
        wait_all(copies(message))
        wait_all(carries(message, c))
        complete(message, c, False)
        ghosts(message, c, "next")
        sweep(c)
        send_local(message + COMPONENTS, c)
        return carry

    lax.fori_loop(0, COMPONENTS * (SWEEPS - 1), turn, 0)

    finals = []

    def give(c, stage_ref, load, out, number):
        for origin in range(2):
            for j in range(local):
                for q in range(half):
                    value = load(origin * local + j, q)
                    at = pl.ds(j, ROWS, stride=local)
                    value = value(stage_ref[origin, q, c, at, :])
                    stage_ref[origin, q, c, at, :] = value
        away = remote(
            stage_ref.at[1 - core, :, c], out.at[mine, c], stage, number, peer
        )
        here = pltpu.make_async_copy(
            stage_ref.at[core, :, c], out.at[mine, c], stage_local.at[number]
        )
        away.start()
        here.start()
        finals.extend([away, here])

    for c in range(COMPONENTS):
        message = COMPONENTS * SWEEPS + c
        wait_all(carries(message, c))
        complete(message, c, True)

        def velocity(t, q, c=c):
            at = pl.ds(t * WIDE + q, ROWS, stride=half)
            return lambda held: held + local_field[c, at, :]

        give(c, stage_iterate, velocity, out_velocity, 2 * COMPONENTS + c)
        wait_all(copies(message))
        ghosts(message, c, "last")
        last_residual(c)

        def remainder(t, q, c=c):
            at = pl.ds(t * CELLS + q, ROWS, stride=half)
            return lambda held: source[c, at, :]

        give(c, stage_forcing, remainder, out_residual, 3 * COMPONENTS + c)
    for copy in finals:
        copy.wait()


def emit(first, second, first_out, second_out, sem):
    copies = [
        pltpu.make_async_copy(first, first_out, sem.at[0]),
        pltpu.make_async_copy(second, second_out, sem.at[1]),
    ]
    for copy in copies:
        copy.start()
    for copy in copies:
        copy.wait()


def body(
    iterate,
    forcing,
    initial_velocity,
    viscosity,
    peclet,
    live_patch_mask,
    neighbour_holder,
    neighbour_slot,
):
    time_devices = lax.axis_size("tm")
    chips = time_devices // 2
    levels = lax.axis_size("space").bit_length() - 1
    slots, local = iterate.shape[:2]
    half = slots // 2
    times = 2 * local

    def by_rows(array):
        split = array.reshape(array.shape[:-1] + (ROWS, LANES))
        if split.ndim == 4:
            return split.transpose(1, 2, 0, 3)
        split = split.transpose(0, 2, 3, 1, 4)
        return split.reshape(slots, COMPONENTS, ROWS * local, LANES)

    def whole(array):
        split = array.reshape(slots, COMPONENTS, ROWS, local, LANES)
        return split.transpose(0, 3, 1, 2, 4).reshape(slots, local, COMPONENTS, ROWS * LANES)

    count = [len(range(d, levels, 3)) for d in range(3)]
    messages = COMPONENTS * (SWEEPS + 1) + 1
    per_message = (chips - 1) + chips * (count[0] + count[1] + 1 + count[2])
    others = max(chips - 1, 1)
    f32 = jnp.float32
    stage = pltpu.VMEM((2, half, COMPONENTS, ROWS * local, LANES), f32)

    def rows(*shape):
        return pltpu.VMEM(shape + (LANES,), f32)

    nx, ny = max(count[0], 1), max(count[1], 1)
    x_rows, y_rows, z_rows = 4 * times + 8, 40, 8 * times + 8
    result = pltpu.VMEM((slots, COMPONENTS, ROWS * local, LANES), f32)
    velocity, residual = pl.pallas_call(
        functools.partial(kernel, (chips, levels, slots, local)),
        out_shape=(result, result),
        in_specs=[pl.BlockSpec(memory_space=pltpu.SMEM)] * 2
        + [pl.BlockSpec(memory_space=pl.ANY)] * 5,
        out_specs=[pl.BlockSpec(memory_space=pl.ANY)] * 2,
        scratch_shapes=[
            stage,
            stage,
            rows(COMPONENTS, times * TALL),
            rows(COMPONENTS, times * WIDE),
            rows(COMPONENTS, times * CELLS),
            rows(COMPONENTS, times * CELLS),
            rows(COMPONENTS, CELLS),
            rows(COMPONENTS, ROWS, slots),
            rows(ROWS, slots),
            rows(COMPONENTS, ROWS, slots),
            rows(COMPONENTS, times * WIDE),
            rows(COMPONENTS, times * 16),
            rows(6, CELLS),
            rows(times * WIDE),
            rows(CELLS),
            rows(chips, CELLS),
            rows(COMPONENTS, CELLS),
            rows(COMPONENTS, CELLS),
            rows(COMPONENTS, CELLS),
            rows(7, 8),
            rows(messages, nx, x_rows),
            rows(messages, nx, x_rows),
            rows(messages, ny, y_rows),
            rows(messages, ny, y_rows),
            rows(messages, 2, z_rows),
            rows(messages, 2, z_rows),
            rows(messages, nx, 4),
            rows(messages, ny, 4),
            rows(messages, nx, others, 4),
            rows(messages, ny, others, 4),
            rows(messages, 2, others, 8),
            rows(messages, others, CELLS),
            rows(nx, chips, 4),
            rows(ny, chips, 4),
            rows(2, chips, 8),
            rows(COMPONENTS, nx, x_rows),
            rows(COMPONENTS, ny, y_rows),
            rows(COMPONENTS, 2, z_rows),
            pltpu.SemaphoreType.DMA((messages * per_message,)),
            pltpu.SemaphoreType.DMA((messages * per_message,)),
            pltpu.SemaphoreType.DMA((4 * COMPONENTS,)),
            pltpu.SemaphoreType.DMA((4 * COMPONENTS,)),
            pltpu.SemaphoreType.DMA((4 * COMPONENTS,)),
            pltpu.SemaphoreType.DMA((3,)),
        ],
        compiler_params=pltpu.CompilerParams(
            collective_id=0, has_side_effects=True, vmem_limit_bytes=121 * 512 * 1024
        ),
    )(
        neighbour_holder,
        live_patch_mask,
        by_rows(iterate),
        by_rows(forcing),
        by_rows(initial_velocity),
        viscosity.reshape(slots, ROWS, LANES).transpose(1, 0, 2),
        by_rows(peclet),
    )
    shape = jax.ShapeDtypeStruct((slots, COMPONENTS, ROWS * local, LANES), f32)
    velocity = pltpu.with_memory_space_constraint(velocity, pltpu.MemorySpace.VMEM)
    residual = pltpu.with_memory_space_constraint(residual, pltpu.MemorySpace.VMEM)
    velocity, residual = pl.pallas_call(
        emit,
        out_shape=(shape, shape),
        in_specs=[pl.BlockSpec(memory_space=pltpu.MemorySpace.VMEM)] * 2,
        out_specs=[pl.BlockSpec(memory_space=pl.ANY)] * 2,
        scratch_shapes=[pltpu.SemaphoreType.DMA((2,))],
        compiler_params=pltpu.CompilerParams(vmem_limit_bytes=4 * 1024 * 1024),
    )(velocity, residual)
    return whole(velocity), whole(residual)


def solution(mesh):
    return jax.shard_map(
        body,
        mesh=mesh,
        in_specs=(
            P("space", "tm", None, None),
            P("space", "tm", None, None),
            P("space", None, None),
            P("space", None),
            P("space", None, None),
            P("space"),
            P("space", None),
            P("space", None),
        ),
        out_specs=(P("space", "tm", None, None), P("space", "tm", None, None)),
        check_vma=False,
    )
```

```python
import functools

import jax
import jax.numpy as jnp
from jax import lax
from jax.experimental import pallas as pl
from jax.experimental.pallas import tpu as pltpu
from jax.sharding import PartitionSpec as P

BLOCK_EDGE = 16
SWEEPS = 5
ALPHA_SCALE = 0.1

ROWS = 32
LANES = 128
COMPONENTS = 3
PLANES = BLOCK_EDGE
CELLS = PLANES * 8
TALL = CELLS + 24
WIDE = CELLS + 8
UNROLL = 16


def kernel(
    dims,
    holder,
    live,
    iterate,
    forcing,
    initial,
    viscosity,
    peclet,
    out_velocity,
    out_residual,
    stage_iterate,
    stage_forcing,
    stage_away,
    field,
    local_field,
    source,
    force,
    start,
    small_initial,
    small_viscosity,
    small_peclet,
    ghost_y,
    ghost_z,
    coefficient,
    power,
    scale,
    gain,
    end_send,
    carry,
    carry_in,
    present,
    x_send,
    x_recv,
    y_send,
    y_recv,
    z_send,
    z_recv,
    x_last,
    y_last,
    y_first_send,
    y_first_recv,
    x_end,
    y_end,
    z_end,
    end_recv,
    x_gain,
    y_gain,
    z_gain,
    x_old,
    y_old,
    z_old,
    send_sem,
    recv_sem,
    stage_send,
    stage_recv,
    stage_local,
    away_sem,
    small_sem,
):
    chips, levels, slots, local = dims
    half = slots // 2
    times = 2 * local
    per_block = 2 * half
    me = lax.axis_index("tm")
    place = lax.axis_index("space")
    chip, core = me // 2, me % 2
    power_message = COMPONENTS * (SWEEPS + 1)

    sub = lax.broadcasted_iota(jnp.int32, (8, LANES), 0)
    lane = lax.broadcasted_iota(jnp.int32, (8, LANES), 1)
    z_index = lane % BLOCK_EDGE
    y_block = lane // BLOCK_EDGE
    y_upper = sub // half == 1
    slot_index = sub % half
    second = slot_index // 2 == 1
    first_block, last_block = y_block == 0, y_block == 7
    z_first, z_last = z_index == 0, z_index == BLOCK_EDGE - 1
    low_inner = (~y_upper) & second
    high_inner = y_upper & (~second)
    flat_lane = lax.broadcasted_iota(jnp.int32, (times, LANES), 1) // BLOCK_EDGE

    place_bit = [place // (1 << b) % 2 for b in range(levels)]

    def links_of(dim):
        found = []
        if dim < levels:
            side = 1 - place_bit[dim]
            if dim + 3 < levels:
                side = 1 - (place_bit[dim] + place_bit[dim + 3]) % 2
            found.append((side, place + (1 << dim) * (1 - 2 * place_bit[dim])))
            if dim + 3 < levels:
                far = dim + 3
                found.append((1 - side, place + (1 << far) * (1 - 2 * place_bit[far])))
        return found

    x_links, y_links, z_links = links_of(0), links_of(1), links_of(2)

    def seat(jump, which):
        return lax.rem(chip + jump, chips) * 2 + which

    greet = [{"tm": seat(j, core)} for j in range(1, chips)]
    for side, partner in x_links + y_links:
        greet += [{"space": partner, "tm": seat(j, core)} for j in range(chips)]
        greet.append({"space": partner, "tm": seat(0, 1 - core)})
    greet += [{"tm": seat(j, 1 - core)} for j in range(chips)]
    for side, partner in z_links:
        greet += [{"space": partner, "tm": seat(j, 1 - core)} for j in range(chips)]
        greet.append({"space": partner})
    barrier = pltpu.get_barrier_semaphore()
    for target in greet:
        pl.semaphore_signal(barrier, inc=1, device_id=target, device_id_type=pl.DeviceIdType.MESH)
    smalls = [
        pltpu.make_async_copy(viscosity, small_viscosity, small_sem.at[0]),
        pltpu.make_async_copy(peclet, small_peclet, small_sem.at[1]),
        pltpu.make_async_copy(initial, small_initial, small_sem.at[2]),
    ]
    for copy in smalls:
        copy.start()

    def remote(src, dst, sems, number, device):
        return pltpu.make_async_remote_copy(
            src_ref=src,
            dst_ref=dst,
            send_sem=sems[0].at[number],
            recv_sem=sems[1].at[number],
            device_id=device,
            device_id_type=pl.DeviceIdType.MESH,
        )

    peer = {"tm": seat(0, 1 - core)}
    mine = pl.ds(core * half, half)
    theirs = pl.ds((1 - core) * half, half)
    stage = (stage_send, stage_recv)
    swaps, owns, aways = [], [], []
    for c in range(COMPONENTS):
        swaps.append(
            remote(iterate.at[theirs, c], stage_iterate.at[core, :, c], stage, c, peer)
        )
        owns.append(
            pltpu.make_async_copy(
                iterate.at[mine, c], stage_iterate.at[core, :, c], stage_local.at[c]
            )
        )
        aways.append(
            pltpu.make_async_copy(iterate.at[theirs, c], stage_away.at[:, c], away_sem.at[c])
        )
        swaps.append(
            remote(forcing.at[theirs, c], stage_forcing.at[core, :, c], stage, COMPONENTS + c, peer)
        )
    for c in range(COMPONENTS):
        owns.append(
            pltpu.make_async_copy(
                forcing.at[mine, c], stage_forcing.at[core, :, c], stage_local.at[COMPONENTS + c]
            )
        )
    for c in range(COMPONENTS):
        owns[c].start()
        aways[c].start()
    for copy in owns[COMPONENTS:]:
        copy.start()

    per_message = (chips - 1) + chips * (len(x_links) + len(y_links) + 1 + len(z_links))

    def collector(message, start):
        sems = (send_sem, recv_sem)
        number = [message * per_message + start]
        found = []

        def add(src, dst, device, condition=None):
            found.append((remote(src, dst, sems, number[0], device), condition))
            number[0] = number[0] + 1

        return found, add

    def faces(message):
        found, add = collector(message, chips - 1)
        last = pl.ds(8 * times, 8)
        for j in range(1, chips):
            for n, (side, partner) in enumerate(x_links):
                add(
                    x_last.at[message, n],
                    x_end.at[message, n, j - 1],
                    {"space": partner, "tm": seat(j, core)},
                )
            for n, (side, partner) in enumerate(y_links):
                add(
                    y_last.at[message, n],
                    y_end.at[message, n, j - 1],
                    {"space": partner, "tm": seat(j, core)},
                )
            for side, partner in z_links:
                add(
                    z_send.at[message, core, last],
                    z_end.at[message, 1 - core, j - 1],
                    {"space": partner, "tm": seat(j, 1 - core)},
                    core == side,
                )
            add(
                z_send.at[message, 1 - core, last],
                z_end.at[message, core, j - 1],
                {"tm": seat(j, 1 - core)},
            )
        return found

    def halos(message):
        found, add = collector(message, per_message - per_message // chips)
        for n, (side, partner) in enumerate(x_links):
            add(x_send.at[message, n], x_recv.at[message, n], {"space": partner})
        for n, (side, partner) in enumerate(y_links):
            add(y_send.at[message, n], y_recv.at[message, n], {"space": partner})
        for side, partner in z_links:
            add(
                z_send.at[message, core],
                z_recv.at[message, 1 - core],
                {"space": partner, "tm": seat(0, 1 - core)},
                core == side,
            )
        add(z_send.at[message, 1 - core], z_recv.at[message, core], peer)
        return found

    def first_copies(c):
        sems = (send_sem, recv_sem)
        number = [c * per_message]
        both, sent, arrived = [], [], []

        def take_number():
            number[0] = number[0] + 1
            return number[0] - 1

        x_size, z_size = 4 * local, 8 * local

        def piece(which, size):
            return pl.ds(pl.multiple_of(which * size, size), size)

        for group in (core, 1 - core):
            for n, (side, partner) in enumerate(x_links):
                both.append(
                    remote(
                        x_send.at[c, n, piece(group, x_size)],
                        x_recv.at[c, n, piece(core, x_size)],
                        sems,
                        take_number(),
                        {"space": partner, "tm": seat(0, group)},
                    )
                )
            for n, (side, partner) in enumerate(y_links):
                both.append(
                    remote(
                        y_first_send.at[c, n, group],
                        y_first_recv.at[c, n, core],
                        sems,
                        take_number(),
                        {"space": partner, "tm": seat(0, group)},
                    )
                )
        for side, partner in z_links:
            numbers = [take_number(), take_number()]

            def outer(index, side=side, partner=partner):
                return remote(
                    z_send.at[c, side, piece(side, z_size)],
                    z_recv.at[c, 1 - side, piece(core, z_size)],
                    sems,
                    index,
                    {"space": partner, "tm": seat(0, 1 - side)},
                )

            sent.append(outer(numbers[0] + core))
            for index in numbers:
                arrived.append((outer(index), core == side))
        both.append(
            remote(
                z_send.at[c, 1 - core, piece(core, z_size)],
                z_recv.at[c, core, piece(core, z_size)],
                sems,
                take_number(),
                peer,
            )
        )
        return both, sent, arrived

    def start_first(c):
        both, sent, arrived = first_copies(c)
        for copy in both + sent:
            copy.start()

    def wait_first(c):
        both, sent, arrived = first_copies(c)
        for copy in both:
            copy.wait()
        for copy in sent:
            copy.wait_send()
        for copy, condition in arrived:
            pl.when(condition)(copy.wait_recv)
        for j in range(local):
            source_row = pl.ds(8 * ((1 - core) * local + j), 8)
            target_row = pl.ds(8 * (core * local + j), 8)
            z_recv[c, 1 - core, target_row, :] = z_send[c, core, source_row, :]
        for n in range(len(y_links)):
            for origin in range(2):
                for k in range(4):
                    value = y_first_recv[c, n, origin, pl.ds(k * local, local), :]
                    y_recv[c, n, pl.ds(8 * k + origin * local, local), :] = value

    def carries(message, c):
        return [
            (
                remote(
                    end_send.at[c],
                    end_recv.at[message, j - 1],
                    (send_sem, recv_sem),
                    message * per_message + j - 1,
                    {"tm": seat(j, core)},
                ),
                None,
            )
            for j in range(1, chips)
        ]

    def start_all(found):
        for copy, condition in found:
            if condition is None:
                copy.start()
            else:
                pl.when(condition)(copy.start)

    def wait_all(found):
        for copy, condition in found:
            if condition is None:
                copy.wait()
            else:
                pl.when(condition)(copy.wait)

    outer_known = functools.reduce(
        jnp.logical_or, [core == side for side, partner in z_links], jnp.bool_(False)
    )

    kept = jnp.where(chip == chips - 1, 0.0, 1.0)

    def pack(message, load, pitch, base, split=False):
        for n, (side, partner) in enumerate(x_links):
            for t in range(times):
                value = load(pl.ds(t * pitch + base + side * (CELLS - 7), 4, stride=2))
                x_send[message, n, pl.ds(4 * t, 4), :] = value
        for n, (side, partner) in enumerate(y_links):
            for k in range(4):
                total = None
                for i in range(8):
                    row = base + ((k % 2) * 8 + i) * 8 + k // 2 + side * 6
                    value = load(pl.ds(row, times, stride=pitch))
                    value = pltpu.roll(value, lax.rem(BLOCK_EDGE * i + 128 - 112 * side, 128), 1)
                    total = value if total is None else jnp.where(flat_lane == i, value, total)
                if split:
                    for group in range(2):
                        part = total[group * local : (group + 1) * local]
                        y_first_send[message, n, group, pl.ds(k * local, local), :] = part
                    continue
                y_send[message, n, pl.ds(8 * k, times), :] = total
        for t in range(times):
            low = high = None
            for x in range(PLANES):
                value = load(pl.ds(t * pitch + base + 8 * x, 8))
                value = pltpu.roll(value, (x - 15) % 128, 1)
                high = value if high is None else jnp.where(z_index == x, value, high)
                low = value if low is None else jnp.where(z_index == (x + 1) % 16, value, low)
            pair = (pltpu.roll(low, 15, 1), high)
            for side in range(2):
                z_send[message, side, pl.ds(8 * t, 8), :] = pair[side]

    def pack_last(message, load):
        for n, (side, partner) in enumerate(x_links):
            value = load(pl.ds(side * (CELLS - 7), 4, stride=2))
            x_last[message, n] = value
            x_send[message, n, pl.ds(4 * times, 4), :] = value
            x_send[message, n, pl.ds(4 * times + 4, 4), :] = value
        for n, (side, partner) in enumerate(y_links):
            for k in range(4):
                value = load(pl.ds(k % 2 * 64 + k // 2 + side * 6, 8, stride=8))
                value = pltpu.roll(value, BLOCK_EDGE * side, 1)
                value = pltpu.roll(value, 0, 1, stride=BLOCK_EDGE, stride_axis=0)
                value = jnp.where(y_block == sub, value, 0.0)
                value = jnp.sum(value, axis=0, keepdims=True)
                y_last[message, n, pl.ds(k, 1), :] = value
                y_send[message, n, pl.ds(32 + k, 1), :] = value
                y_send[message, n, pl.ds(36 + k, 1), :] = value
        low = high = None
        for x in range(PLANES):
            value = pltpu.roll(load(pl.ds(8 * x, 8)), (x - 15) % 128, 1)
            high = value if high is None else jnp.where(z_index == x, value, high)
            low = value if low is None else jnp.where(z_index == (x + 1) % 16, value, low)
        z_send[message, 0, pl.ds(8 * times, 8), :] = pltpu.roll(low, 15, 1)
        z_send[message, 1, pl.ds(8 * times, 8), :] = high

    wraps = [jnp.where(chip - j < 0, ALPHA_SCALE, 1.0) for j in range(1, chips + 1)]
    def gains_of(ratio):
        powers = [jnp.ones_like(ratio)]
        for j in range(chips):
            powers.append(powers[-1] * ratio)
        scaled = 1.0 / (1.0 - ALPHA_SCALE * powers[chips])
        return [wraps[j] * (powers[j] * scaled) for j in range(chips)]

    def combine(gains, ends):
        total = gains[0] * ends[0]
        for j in range(1, chips):
            total = total + gains[j] * ends[j]
        return total

    def x_ends(message, n):
        found = [x_end[message, n, j] for j in range(chips - 1)]
        return found + [x_recv[message, n, pl.ds(4 * times, 4), :]]

    def y_ends(message, n):
        found = [y_end[message, n, j] for j in range(chips - 1)]
        return found + [y_recv[message, n, pl.ds(32, 4), :]]

    def z_ends(message, side):
        found = [z_end[message, side, j] for j in range(chips - 1)]
        return found + [z_recv[message, side, pl.ds(8 * times, 8), :]]

    def ghosts(message, c, mode):
        def finish(value, old, index):
            if mode == "raw":
                return value
            if mode == "last":
                return value - old[index]
            old[index] = value
            return value

        for t in range(times):
            base = t * TALL
            field[c, pl.ds(base, 8), :] = field[c, pl.ds(base + CELLS - 1, 8), :]
            field[c, pl.ds(base + CELLS + 8, 8), :] = field[c, pl.ds(base + 9, 8), :]
        for n, (side, partner) in enumerate(x_links):
            if mode != "raw":
                added = combine([x_gain[n, j] for j in range(chips)], x_ends(message, n))
            for t in range(times):
                at = pl.ds(4 * t, 4)
                value = x_recv[message, n, at, :]
                if mode != "raw":
                    value = value + x_recv[power_message, n, at, :] * added
                value = finish(value, x_old, (c, n, at, slice(None)))
                field[c, pl.ds(t * TALL + side * (CELLS + 9), 4, stride=2), :] = value
        for n, (side, partner) in enumerate(y_links):
            if mode != "raw":
                added = combine([y_gain[n, j] for j in range(chips)], y_ends(message, n))
            for k in range(4):
                at = pl.ds(8 * k, times)
                value = y_recv[message, n, at, :]
                if mode != "raw":
                    value = value + y_recv[power_message, n, at, :] * added[k : k + 1]
                value = finish(value, y_old, (c, n, at, slice(None)))
                for i in range(8):
                    turned = pltpu.roll(
                        value, lax.rem(112 * (1 - side) + 128 - BLOCK_EDGE * i, 128), 1
                    )
                    row = ((k % 2) * 8 + i) * 8 + k // 2 + side * 6
                    ghost_y[c, pl.ds(row, times, stride=WIDE), :] = turned
        added = [None, None]
        for side in range(2):
            if mode != "raw":
                gains = [z_gain[side, j] for j in range(chips)]
                added[side] = combine(gains, z_ends(message, side))
        even = z_index % 2 == 0
        for t in range(times):
            at = pl.ds(8 * t, 8)
            pair = []
            for side in range(2):
                value = z_recv[message, side, at, :]
                if mode != "raw":
                    value = value + z_recv[power_message, side, at, :] * added[side]
                value = jnp.where((core != side) | outer_known, value, 0.0)
                pair.append(finish(value, z_old, (c, side, at, slice(None))))
            low, high = pair[0], pltpu.roll(pair[1], 15, 1)
            ghost_z[c, pl.ds(16 * t, 8), :] = jnp.where(even, low, high)
            ghost_z[c, pl.ds(16 * t + 8, 8), :] = jnp.where(even, high, low)

    def stencil(c, t, x, row, parity, factors):
        base = t * TALL + 8 + row

        def load(shift):
            return field[c, pl.ds(base + shift, 8), :]

        value = load(0)
        total = factors[0] * load(-8) + factors[1] * load(8)
        beyond = ghost_y[c, pl.ds(t * WIDE + row, 8), :]
        low = jnp.where(y_upper, load(-4), jnp.where(low_inner, load(2), beyond))
        low = pltpu.roll(jnp.where(last_block, low, value), 16, 1)
        high = jnp.where(y_upper, jnp.where(high_inner, load(-2), beyond), load(4))
        high = pltpu.roll(jnp.where(first_block, high, value), 112, 1)
        total = total + factors[2] * low + factors[3] * high
        edge = ghost_z[c, pl.ds(16 * t + 8 * parity, 8), :]
        edge = pltpu.roll(edge, lax.rem(128 - x, 128), 1)
        low = jnp.where(z_first, edge, pltpu.roll(value, 1, 1))
        high = jnp.where(z_last, edge, pltpu.roll(value, 127, 1))
        return value, total + factors[4] * low + factors[5] * high

    def over_planes(body):
        def one(group, carry):
            for i in range(UNROLL):
                x = group * UNROLL + i
                body(x, pl.multiple_of(x * 8, 8), i % 2)
            return carry

        lax.fori_loop(0, PLANES // UNROLL, one, 0)

    def factors_at(row):
        return [coefficient[f, pl.ds(row, 8), :] for f in range(6)]

    def sweep(c):
        def plane(x, row, parity):
            factors = factors_at(row)
            ratio = power[pl.ds(row, 8), :]
            before = None
            for t in range(times):
                _, total = stencil(c, t, x, row, parity, factors)
                total = total + source[c, pl.ds(t * CELLS + row, 8), :]
                if before is not None:
                    total = total + ratio * before
                local_field[c, pl.ds(t * WIDE + row, 8), :] = total
                before = total
            end_send[c, pl.ds(row, 8), :] = before + carry[c, pl.ds(row, 8), :]

        over_planes(plane)

    def first_residual(c):
        def plane(x, row, parity):
            factors = factors_at(row)
            ratio = power[pl.ds(row, 8), :]
            inverse = scale[pl.ds(row, 8), :]
            alive = present[6]
            earlier = jnp.where(chip == 0, start[c, pl.ds(row, 8), :], 0.0)
            before = None
            for t in range(times):
                value, total = stencil(c, t, x, row, parity, factors)
                total = total + inverse * force[c, pl.ds(t * CELLS + row, 8), :]
                total = (total + (ratio * earlier - value)) * alive
                source[c, pl.ds(t * CELLS + row, 8), :] = total
                if before is not None:
                    total = total + ratio * before
                local_field[c, pl.ds(t * WIDE + row, 8), :] = total
                before, earlier = total, value
            kept_end = kept * (earlier * alive)
            carry[c, pl.ds(row, 8), :] = kept_end
            end_send[c, pl.ds(row, 8), :] = before + kept_end

        over_planes(plane)

    def complete(message, c, last):
        def plane(x, row, parity):
            ends = [end_recv[message, j, pl.ds(row, 8), :] for j in range(chips - 1)]
            ends.append(end_send[c, pl.ds(row, 8), :])
            gains = [gain[j, pl.ds(row, 8), :] for j in range(chips)]
            added = combine(gains, ends)
            if last:
                carry_in[c, pl.ds(row, 8), :] = added
            for t in range(times):
                value = local_field[c, pl.ds(t * WIDE + row, 8), :]
                value = value + power[pl.ds(t * WIDE + row, 8), :] * added
                at = pl.ds(t * TALL + 8 + row, 8)
                if last:
                    local_field[c, pl.ds(t * WIDE + row, 8), :] = value
                    value = value - field[c, at, :]
                field[c, at, :] = value

        over_planes(plane)

    def last_residual(c):
        def plane(x, row, parity):
            factors = factors_at(row)
            diagonal = 1.0 / scale[pl.ds(row, 8), :]
            for t in range(times):
                _, total = stencil(c, t, x, row, parity, factors)
                total = total * diagonal
                if t == 0:
                    added = carry_in[c, pl.ds(row, 8), :]
                    total = total - jnp.where(chip == 0, 2.0 * added, 0.0)
                source[c, pl.ds(t * CELLS + row, 8), :] = total

        over_planes(plane)

    def take(stage_ref, origin, store):
        for j in range(local):
            for q in range(half):
                store(origin * local + j, q, stage_ref[q, pl.ds(j, ROWS, stride=local), :])

    def scatter(value, target, q):
        target[pl.ds(q, ROWS, stride=half), :] = value

    for copy in smalls:
        copy.wait()
    for q in range(half):
        slot = core * half + q
        scatter(small_viscosity[:, slot, :], scale, q)
        for d in range(3):
            scatter(small_peclet[d, :, slot, :], coefficient.at[2 * d], q)
        for c in range(COMPONENTS):
            scatter(small_initial[c, :, slot, :], start.at[c], q)
    for f in range(7):
        value = jnp.zeros((8, LANES), jnp.float32)
        for q in range(half):
            slot = core * half + q
            known = live[slot] > 0 if f == 6 else holder[slot, f] >= 0
            value = jnp.where(slot_index == q, jnp.where(known, 1.0, 0.0), value)
        present[f] = value

    def make(x, row, parity):
        at = pl.ds(row, 8)
        thickness = scale[at, :]
        inverse = 1.0 / (2.0 + 6.0 * thickness)
        scale[at, :] = inverse
        weight = thickness * inverse
        edges = [
            x == 0,
            x == PLANES - 1,
            (~y_upper) & first_block,
            y_upper & last_block,
            z_first,
            z_last,
        ]
        for d in range(3):
            number = coefficient[2 * d, at, :]
            for f, factor in ((2 * d, 1.0 + number), (2 * d + 1, 1.0 - number)):
                slot_edge = edges[f]
                value = weight * factor
                coefficient[f, at, :] = jnp.where(slot_edge, value * present[f], value)
        ratio = 2.0 * inverse
        total = ratio
        for t in range(times):
            power[pl.ds(t * WIDE + row, 8), :] = total
            if t == times - 1:
                for j, value in enumerate(gains_of(total)):
                    gain[j, at, :] = value
            total = total * ratio

    over_planes(make)
    ghost_y[...] = jnp.zeros_like(ghost_y)

    pack(power_message, lambda at: power[at, :], WIDE, 0)
    power_last = (times - 1) * WIDE
    pack_last(power_message, lambda at: power[pl.ds(power_last + at.start, at.size, at.stride), :])

    def offer(c):
        owns[c].wait()
        aways[c].wait()

        def store_both(t, q, value):
            field[c, pl.ds(t * TALL + 8 + q, ROWS, stride=half), :] = value
            local_field[c, pl.ds(t * WIDE + q, ROWS, stride=half), :] = value

        def store_away(t, q, value):
            local_field[c, pl.ds(t * WIDE + q, ROWS, stride=half), :] = value

        take(stage_iterate.at[core, :, c], core, store_both)
        take(stage_away.at[:, c], 1 - core, store_away)
        pack(c, lambda at: local_field[c, at, :], WIDE, 0, split=True)

    offer(0)
    pl.semaphore_wait(barrier, len(greet))
    start_first(0)
    for copy in swaps:
        copy.start()
    power_copies = halos(power_message)
    start_all(power_copies)
    for c in range(1, COMPONENTS):
        offer(c)
        start_first(c)

    def send_local(message, c):
        pack_last(message, lambda at: end_send[c, at, :])
        start_all(faces(message))
        start_all(carries(message, c))
        pack(message, lambda at: local_field[c, at, :], WIDE, 0)
        start_all(halos(message))

    def opening(c):
        swaps[2 * c].wait()
        swaps[2 * c + 1].wait()
        owns[COMPONENTS + c].wait()

        def store(t, q, value):
            field[c, pl.ds(t * TALL + 8 + q, ROWS, stride=half), :] = value

        def store_force(t, q, value):
            force[c, pl.ds(t * CELLS + q, ROWS, stride=half), :] = value

        take(stage_iterate.at[1 - core, :, c], 1 - core, store)
        for origin in range(2):
            take(stage_forcing.at[origin, :, c], origin, store_force)
        wait_first(c)
        ghosts(c, c, "raw")
        first_residual(c)
        send_local(COMPONENTS + c, c)

    for c in range(COMPONENTS):
        opening(c)
    wait_all(power_copies)
    for n in range(len(x_links)):
        for j, value in enumerate(gains_of(x_recv[power_message, n, pl.ds(4 * times, 4), :])):
            x_gain[n, j] = value
    for n in range(len(y_links)):
        for j, value in enumerate(gains_of(y_recv[power_message, n, pl.ds(32, 4), :])):
            y_gain[n, j] = value
    for side in range(2):
        ratio = z_recv[power_message, side, pl.ds(8 * times, 8), :]
        for j, value in enumerate(gains_of(ratio)):
            z_gain[side, j] = value

    def turn(step, carry):
        c = lax.rem(step, COMPONENTS)
        message = COMPONENTS + step
        wait_all(halos(message))
        wait_all(faces(message))
        wait_all(carries(message, c))
        complete(message, c, False)
        ghosts(message, c, "next")
        sweep(c)
        send_local(message + COMPONENTS, c)
        return carry

    lax.fori_loop(0, COMPONENTS * (SWEEPS - 1), turn, 0)

    finals = []

    def give(c, stage_ref, load, out, number):
        for origin in range(2):
            for j in range(local):
                for q in range(half):
                    value = load(origin * local + j, q)
                    at = pl.ds(j, ROWS, stride=local)
                    value = value(stage_ref[origin, q, c, at, :])
                    stage_ref[origin, q, c, at, :] = value
        away = remote(
            stage_ref.at[1 - core, :, c], out.at[mine, c], stage, number, peer
        )
        here = pltpu.make_async_copy(
            stage_ref.at[core, :, c], out.at[mine, c], stage_local.at[number]
        )
        away.start()
        here.start()
        finals.extend([away, here])

    for c in range(COMPONENTS):
        message = COMPONENTS * SWEEPS + c
        wait_all(carries(message, c))
        complete(message, c, True)

        def velocity(t, q, c=c):
            at = pl.ds(t * WIDE + q, ROWS, stride=half)
            return lambda held: held + local_field[c, at, :]

        give(c, stage_iterate, velocity, out_velocity, 2 * COMPONENTS + c)
        wait_all(halos(message))
        wait_all(faces(message))
        ghosts(message, c, "last")
        last_residual(c)

        def remainder(t, q, c=c):
            at = pl.ds(t * CELLS + q, ROWS, stride=half)
            return lambda held: source[c, at, :]

        give(c, stage_forcing, remainder, out_residual, 3 * COMPONENTS + c)
    for copy in finals:
        copy.wait()


def emit(first, second, first_out, second_out, sem):
    copies = [
        pltpu.make_async_copy(first, first_out, sem.at[0]),
        pltpu.make_async_copy(second, second_out, sem.at[1]),
    ]
    for copy in copies:
        copy.start()
    for copy in copies:
        copy.wait()


def body(
    iterate,
    forcing,
    initial_velocity,
    viscosity,
    peclet,
    live_patch_mask,
    neighbour_holder,
    neighbour_slot,
):
    time_devices = lax.axis_size("tm")
    chips = time_devices // 2
    levels = lax.axis_size("space").bit_length() - 1
    slots, local = iterate.shape[:2]
    half = slots // 2
    times = 2 * local

    def by_rows(array):
        split = array.reshape(array.shape[:-1] + (ROWS, LANES))
        if split.ndim == 4:
            return split.transpose(1, 2, 0, 3)
        split = split.transpose(0, 2, 3, 1, 4)
        return split.reshape(slots, COMPONENTS, ROWS * local, LANES)

    def whole(array):
        split = array.reshape(slots, COMPONENTS, ROWS, local, LANES)
        return split.transpose(0, 3, 1, 2, 4).reshape(slots, local, COMPONENTS, ROWS * LANES)

    count = [len(range(d, levels, 3)) for d in range(3)]
    messages = COMPONENTS * (SWEEPS + 1) + 1
    per_message = (chips - 1) + chips * (count[0] + count[1] + 1 + count[2])
    others = max(chips - 1, 1)
    f32 = jnp.float32
    stage = pltpu.VMEM((2, half, COMPONENTS, ROWS * local, LANES), f32)

    def rows(*shape):
        return pltpu.VMEM(shape + (LANES,), f32)

    nx, ny = max(count[0], 1), max(count[1], 1)
    x_rows, y_rows, z_rows = 4 * times + 8, 40, 8 * times + 8
    result = pltpu.VMEM((slots, COMPONENTS, ROWS * local, LANES), f32)
    velocity, residual = pl.pallas_call(
        functools.partial(kernel, (chips, levels, slots, local)),
        out_shape=(result, result),
        in_specs=[pl.BlockSpec(memory_space=pltpu.SMEM)] * 2
        + [pl.BlockSpec(memory_space=pl.ANY)] * 5,
        out_specs=[pl.BlockSpec(memory_space=pl.ANY)] * 2,
        scratch_shapes=[
            stage,
            stage,
            pltpu.VMEM((half, COMPONENTS, ROWS * local, LANES), f32),
            rows(COMPONENTS, times * TALL),
            rows(COMPONENTS, times * WIDE),
            rows(COMPONENTS, times * CELLS),
            rows(COMPONENTS, times * CELLS),
            rows(COMPONENTS, CELLS),
            rows(COMPONENTS, ROWS, slots),
            rows(ROWS, slots),
            rows(COMPONENTS, ROWS, slots),
            rows(COMPONENTS, times * WIDE),
            rows(COMPONENTS, times * 16),
            rows(6, CELLS),
            rows(times * WIDE),
            rows(CELLS),
            rows(chips, CELLS),
            rows(COMPONENTS, CELLS),
            rows(COMPONENTS, CELLS),
            rows(COMPONENTS, CELLS),
            rows(7, 8),
            rows(messages, nx, x_rows),
            rows(messages, nx, x_rows),
            rows(messages, ny, y_rows),
            rows(messages, ny, y_rows),
            rows(messages, 2, z_rows),
            rows(messages, 2, z_rows),
            rows(messages, nx, 4),
            rows(messages, ny, 4),
            rows(COMPONENTS, ny, 2, 4 * local),
            rows(COMPONENTS, ny, 2, 4 * local),
            rows(messages, nx, others, 4),
            rows(messages, ny, others, 4),
            rows(messages, 2, others, 8),
            rows(messages, others, CELLS),
            rows(nx, chips, 4),
            rows(ny, chips, 4),
            rows(2, chips, 8),
            rows(COMPONENTS, nx, x_rows),
            rows(COMPONENTS, ny, y_rows),
            rows(COMPONENTS, 2, z_rows),
            pltpu.SemaphoreType.DMA((messages * per_message,)),
            pltpu.SemaphoreType.DMA((messages * per_message,)),
            pltpu.SemaphoreType.DMA((4 * COMPONENTS,)),
            pltpu.SemaphoreType.DMA((4 * COMPONENTS,)),
            pltpu.SemaphoreType.DMA((4 * COMPONENTS,)),
            pltpu.SemaphoreType.DMA((COMPONENTS,)),
            pltpu.SemaphoreType.DMA((3,)),
        ],
        compiler_params=pltpu.CompilerParams(
            collective_id=0, has_side_effects=True, vmem_limit_bytes=121 * 512 * 1024
        ),
    )(
        neighbour_holder,
        live_patch_mask,
        by_rows(iterate),
        by_rows(forcing),
        by_rows(initial_velocity),
        viscosity.reshape(slots, ROWS, LANES).transpose(1, 0, 2),
        by_rows(peclet),
    )
    shape = jax.ShapeDtypeStruct((slots, COMPONENTS, ROWS * local, LANES), f32)
    velocity = pltpu.with_memory_space_constraint(velocity, pltpu.MemorySpace.VMEM)
    residual = pltpu.with_memory_space_constraint(residual, pltpu.MemorySpace.VMEM)
    velocity, residual = pl.pallas_call(
        emit,
        out_shape=(shape, shape),
        in_specs=[pl.BlockSpec(memory_space=pltpu.MemorySpace.VMEM)] * 2,
        out_specs=[pl.BlockSpec(memory_space=pl.ANY)] * 2,
        scratch_shapes=[pltpu.SemaphoreType.DMA((2,))],
        compiler_params=pltpu.CompilerParams(vmem_limit_bytes=4 * 1024 * 1024),
    )(velocity, residual)
    return whole(velocity), whole(residual)


def solution(mesh):
    return jax.shard_map(
        body,
        mesh=mesh,
        in_specs=(
            P("space", "tm", None, None),
            P("space", "tm", None, None),
            P("space", None, None),
            P("space", None),
            P("space", None, None),
            P("space"),
            P("space", None),
            P("space", None),
        ),
        out_specs=(P("space", "tm", None, None), P("space", "tm", None, None)),
        check_vma=False,
    )
```

```python
import functools

import jax
import jax.numpy as jnp
from jax import lax
from jax.experimental import pallas as pl
from jax.experimental.pallas import tpu as pltpu
from jax.sharding import PartitionSpec as P

BLOCK_EDGE = 16
SWEEPS = 5
ALPHA_SCALE = 0.1

ROWS = 32
LANES = 128
COMPONENTS = 3
PLANES = BLOCK_EDGE
CELLS = PLANES * 8
TALL = CELLS + 24
WIDE = CELLS + 8
UNROLL = 16
ONCE = 16


def kernel(
    dims,
    holder,
    live,
    iterate,
    forcing,
    initial,
    viscosity,
    peclet,
    out_velocity,
    out_residual,
    stage_iterate,
    stage_forcing,
    stage_away,
    field,
    local_field,
    source,
    force,
    start,
    small_initial,
    small_viscosity,
    small_peclet,
    ghost_y,
    ghost_z,
    coefficient,
    power,
    scale,
    gain,
    end_send,
    carry,
    carry_in,
    present,
    x_send,
    x_recv,
    y_send,
    y_recv,
    z_send,
    z_recv,
    x_last,
    y_last,
    y_first_send,
    y_first_recv,
    x_end,
    y_end,
    z_end,
    end_recv,
    x_gain,
    y_gain,
    z_gain,
    x_old,
    y_old,
    z_old,
    send_sem,
    recv_sem,
    stage_send,
    stage_recv,
    stage_local,
    away_sem,
    small_sem,
):
    chips, levels, slots, local = dims
    half = slots // 2
    times = 2 * local
    per_block = 2 * half
    me = lax.axis_index("tm")
    place = lax.axis_index("space")
    chip, core = me // 2, me % 2
    power_message = COMPONENTS * (SWEEPS + 1)

    sub = lax.broadcasted_iota(jnp.int32, (8, LANES), 0)
    lane = lax.broadcasted_iota(jnp.int32, (8, LANES), 1)
    z_index = lane % BLOCK_EDGE
    y_block = lane // BLOCK_EDGE
    y_upper = sub // half == 1
    slot_index = sub % half
    second = slot_index // 2 == 1
    first_block, last_block = y_block == 0, y_block == 7
    z_first, z_last = z_index == 0, z_index == BLOCK_EDGE - 1
    low_inner = (~y_upper) & second
    high_inner = y_upper & (~second)
    flat_lane = lax.broadcasted_iota(jnp.int32, (times, LANES), 1) // BLOCK_EDGE

    place_bit = [place // (1 << b) % 2 for b in range(levels)]

    def links_of(dim):
        found = []
        if dim < levels:
            side = 1 - place_bit[dim]
            if dim + 3 < levels:
                side = 1 - (place_bit[dim] + place_bit[dim + 3]) % 2
            found.append((side, place + (1 << dim) * (1 - 2 * place_bit[dim])))
            if dim + 3 < levels:
                far = dim + 3
                found.append((1 - side, place + (1 << far) * (1 - 2 * place_bit[far])))
        return found

    x_links, y_links, z_links = links_of(0), links_of(1), links_of(2)

    bases = [lax.rem(chip + jump, chips) * 2 for jump in range(chips)]

    def seat(jump, which):
        return bases[jump] + which

    greet = [{"tm": seat(j, core)} for j in range(1, chips)]
    for side, partner in x_links + y_links:
        greet += [{"space": partner, "tm": seat(j, core)} for j in range(chips)]
        greet.append({"space": partner, "tm": seat(0, 1 - core)})
    greet += [{"tm": seat(j, 1 - core)} for j in range(chips)]
    for side, partner in z_links:
        greet += [{"space": partner, "tm": seat(j, 1 - core)} for j in range(chips)]
        greet.append({"space": partner})
    barrier = pltpu.get_barrier_semaphore()
    for target in greet:
        pl.semaphore_signal(barrier, inc=1, device_id=target, device_id_type=pl.DeviceIdType.MESH)
    smalls = [
        pltpu.make_async_copy(viscosity, small_viscosity, small_sem.at[0]),
        pltpu.make_async_copy(peclet, small_peclet, small_sem.at[1]),
        pltpu.make_async_copy(initial, small_initial, small_sem.at[2]),
    ]
    for copy in smalls:
        copy.start()

    def remote(src, dst, sems, number, device):
        return pltpu.make_async_remote_copy(
            src_ref=src,
            dst_ref=dst,
            send_sem=sems[0].at[number],
            recv_sem=sems[1].at[number],
            device_id=device,
            device_id_type=pl.DeviceIdType.MESH,
        )

    peer = {"tm": seat(0, 1 - core)}
    mine = pl.ds(core * half, half)
    theirs = pl.ds((1 - core) * half, half)
    stage = (stage_send, stage_recv)

    def swaps(c):
        return [
            remote(iterate.at[theirs, c], stage_iterate.at[core, :, c], stage, c, peer),
            remote(forcing.at[theirs, c], stage_forcing.at[core, :, c], stage, COMPONENTS + c, peer),
        ]

    def owns(c):
        return [
            pltpu.make_async_copy(
                iterate.at[mine, c], stage_iterate.at[core, :, c], stage_local.at[c]
            ),
            pltpu.make_async_copy(iterate.at[theirs, c], stage_away.at[:, c], away_sem.at[c]),
        ]

    def own_forcing(c):
        return pltpu.make_async_copy(
            forcing.at[mine, c], stage_forcing.at[core, :, c], stage_local.at[COMPONENTS + c]
        )

    for c in range(COMPONENTS):
        for copy in owns(c):
            copy.start()
    for c in range(COMPONENTS):
        own_forcing(c).start()

    per_message = (chips - 1) + chips * (len(x_links) + len(y_links) + 1 + len(z_links))

    def collector(message, start):
        sems = (send_sem, recv_sem)
        number = [message * per_message + start]
        found = []

        def add(src, dst, device, condition=None):
            found.append((remote(src, dst, sems, number[0], device), condition))
            number[0] = number[0] + 1

        return found, add

    def faces(message):
        found, add = collector(message, chips - 1)
        last = pl.ds(8 * times, 8)
        for j in range(1, chips):
            for n, (side, partner) in enumerate(x_links):
                add(
                    x_last.at[message, n],
                    x_end.at[message, n, j - 1],
                    {"space": partner, "tm": seat(j, core)},
                )
            for n, (side, partner) in enumerate(y_links):
                add(
                    y_last.at[message, n],
                    y_end.at[message, n, j - 1],
                    {"space": partner, "tm": seat(j, core)},
                )
            for side, partner in z_links:
                add(
                    z_send.at[message, core, last],
                    z_end.at[message, 1 - core, j - 1],
                    {"space": partner, "tm": seat(j, 1 - core)},
                    core == side,
                )
            add(
                z_send.at[message, 1 - core, last],
                z_end.at[message, core, j - 1],
                {"tm": seat(j, 1 - core)},
            )
        return found

    def halos(message):
        found, add = collector(message, per_message - per_message // chips)
        for n, (side, partner) in enumerate(x_links):
            add(x_send.at[message, n], x_recv.at[message, n], {"space": partner})
        for n, (side, partner) in enumerate(y_links):
            add(y_send.at[message, n], y_recv.at[message, n], {"space": partner})
        for side, partner in z_links:
            add(
                z_send.at[message, core],
                z_recv.at[message, 1 - core],
                {"space": partner, "tm": seat(0, 1 - core)},
                core == side,
            )
        add(z_send.at[message, 1 - core], z_recv.at[message, core], peer)
        return found

    def first_copies(c):
        sems = (send_sem, recv_sem)
        number = [c * per_message]
        both, sent, arrived = [], [], []

        def take_number():
            number[0] = number[0] + 1
            return number[0] - 1

        x_size, z_size = 4 * local, 8 * local

        def piece(which, size):
            return pl.ds(pl.multiple_of(which * size, size), size)

        for group in (core, 1 - core):
            for n, (side, partner) in enumerate(x_links):
                both.append(
                    remote(
                        x_send.at[c, n, piece(group, x_size)],
                        x_recv.at[c, n, piece(core, x_size)],
                        sems,
                        take_number(),
                        {"space": partner, "tm": seat(0, group)},
                    )
                )
            for n, (side, partner) in enumerate(y_links):
                both.append(
                    remote(
                        y_first_send.at[c, n, group],
                        y_first_recv.at[c, n, core],
                        sems,
                        take_number(),
                        {"space": partner, "tm": seat(0, group)},
                    )
                )
        for side, partner in z_links:
            numbers = [take_number(), take_number()]

            def outer(index, side=side, partner=partner):
                return remote(
                    z_send.at[c, side, piece(side, z_size)],
                    z_recv.at[c, 1 - side, piece(core, z_size)],
                    sems,
                    index,
                    {"space": partner, "tm": seat(0, 1 - side)},
                )

            sent.append(outer(numbers[0] + core))
            for index in numbers:
                arrived.append((outer(index), core == side))
        both.append(
            remote(
                z_send.at[c, 1 - core, piece(core, z_size)],
                z_recv.at[c, core, piece(core, z_size)],
                sems,
                take_number(),
                peer,
            )
        )
        return both, sent, arrived

    def start_first(c):
        both, sent, arrived = first_copies(c)
        for copy in both + sent:
            copy.start()

    def wait_first(c):
        both, sent, arrived = first_copies(c)
        for copy in both:
            copy.wait()
        for copy in sent:
            copy.wait_send()
        for copy, condition in arrived:
            pl.when(condition)(copy.wait_recv)
        for j in range(local):
            source_row = pl.ds(8 * ((1 - core) * local + j), 8)
            target_row = pl.ds(8 * (core * local + j), 8)
            z_recv[c, 1 - core, target_row, :] = z_send[c, core, source_row, :]
        for n in range(len(y_links)):
            for origin in range(2):
                for k in range(4):
                    value = y_first_recv[c, n, origin, pl.ds(k * local, local), :]
                    y_recv[c, n, pl.ds(8 * k + origin * local, local), :] = value

    def carries(message, c):
        return [
            (
                remote(
                    end_send.at[c],
                    end_recv.at[message, j - 1],
                    (send_sem, recv_sem),
                    message * per_message + j - 1,
                    {"tm": seat(j, core)},
                ),
                None,
            )
            for j in range(1, chips)
        ]

    def start_all(found):
        for copy, condition in found:
            if condition is None:
                copy.start()
            else:
                pl.when(condition)(copy.start)

    def wait_all(found):
        for copy, condition in found:
            if condition is None:
                copy.wait()
            else:
                pl.when(condition)(copy.wait)

    outer_known = functools.reduce(
        jnp.logical_or, [core == side for side, partner in z_links], jnp.bool_(False)
    )

    kept = jnp.where(chip == chips - 1, 0.0, 1.0)

    def pack_x(message, load, pitch, base):
        for n, (side, partner) in enumerate(x_links):
            for t in range(times):
                value = load(pl.ds(t * pitch + base + side * (CELLS - 7), 4, stride=2))
                x_send[message, n, pl.ds(4 * t, 4), :] = value

    def pack_y(message, load, pitch, base, split=False):
        for n, (side, partner) in enumerate(y_links):
            for k in range(4):
                total = None
                for i in range(8):
                    row = base + ((k % 2) * 8 + i) * 8 + k // 2 + side * 6
                    value = load(pl.ds(row, times, stride=pitch))
                    value = pltpu.roll(value, lax.rem(BLOCK_EDGE * i + 128 - 112 * side, 128), 1)
                    total = value if total is None else jnp.where(flat_lane == i, value, total)
                if split:
                    for group in range(2):
                        part = total[group * local : (group + 1) * local]
                        y_first_send[message, n, group, pl.ds(k * local, local), :] = part
                    continue
                y_send[message, n, pl.ds(8 * k, times), :] = total

    def pack_z(message, load, pitch, base):
        for t in range(times):
            low = high = None
            for x in range(PLANES):
                value = load(pl.ds(t * pitch + base + 8 * x, 8))
                value = pltpu.roll(value, (x - 15) % 128, 1)
                high = value if high is None else jnp.where(z_index == x, value, high)
                low = value if low is None else jnp.where(z_index == (x + 1) % 16, value, low)
            pair = (pltpu.roll(low, 15, 1), high)
            for side in range(2):
                z_send[message, side, pl.ds(8 * t, 8), :] = pair[side]

    def pack(message, load, pitch, base, split=False):
        pack_z(message, load, pitch, base)
        pack_y(message, load, pitch, base, split)
        pack_x(message, load, pitch, base)

    def pack_last(message, load):
        for n, (side, partner) in enumerate(x_links):
            value = load(pl.ds(side * (CELLS - 7), 4, stride=2))
            x_last[message, n] = value
            x_send[message, n, pl.ds(4 * times, 4), :] = value
            x_send[message, n, pl.ds(4 * times + 4, 4), :] = value
        for n, (side, partner) in enumerate(y_links):
            for k in range(4):
                value = load(pl.ds(k % 2 * 64 + k // 2 + side * 6, 8, stride=8))
                value = pltpu.roll(value, BLOCK_EDGE * side, 1)
                value = pltpu.roll(value, 0, 1, stride=BLOCK_EDGE, stride_axis=0)
                value = jnp.where(y_block == sub, value, 0.0)
                value = jnp.sum(value, axis=0, keepdims=True)
                y_last[message, n, pl.ds(k, 1), :] = value
                y_send[message, n, pl.ds(32 + k, 1), :] = value
                y_send[message, n, pl.ds(36 + k, 1), :] = value
        low = high = None
        for x in range(PLANES):
            value = pltpu.roll(load(pl.ds(8 * x, 8)), (x - 15) % 128, 1)
            high = value if high is None else jnp.where(z_index == x, value, high)
            low = value if low is None else jnp.where(z_index == (x + 1) % 16, value, low)
        z_send[message, 0, pl.ds(8 * times, 8), :] = pltpu.roll(low, 15, 1)
        z_send[message, 1, pl.ds(8 * times, 8), :] = high

    wraps = [jnp.where(chip - j < 0, ALPHA_SCALE, 1.0) for j in range(1, chips + 1)]
    def gains_of(ratio):
        powers = [jnp.ones_like(ratio)]
        for j in range(chips):
            powers.append(powers[-1] * ratio)
        scaled = 1.0 / (1.0 - ALPHA_SCALE * powers[chips])
        return [wraps[j] * (powers[j] * scaled) for j in range(chips)]

    def combine(gains, ends):
        total = gains[0] * ends[0]
        for j in range(1, chips):
            total = total + gains[j] * ends[j]
        return total

    def x_ends(message, n):
        found = [x_end[message, n, j] for j in range(chips - 1)]
        return found + [x_recv[message, n, pl.ds(4 * times, 4), :]]

    def y_ends(message, n):
        found = [y_end[message, n, j] for j in range(chips - 1)]
        return found + [y_recv[message, n, pl.ds(32, 4), :]]

    def z_ends(message, side):
        found = [z_end[message, side, j] for j in range(chips - 1)]
        return found + [z_recv[message, side, pl.ds(8 * times, 8), :]]

    def ghosts(message, c, mode):
        def finish(value, old, index):
            if mode == "raw":
                return value
            if mode == "last":
                return value - old[index]
            old[index] = value
            return value

        for t in range(times):
            base = t * TALL
            field[c, pl.ds(base, 8), :] = field[c, pl.ds(base + CELLS - 1, 8), :]
            field[c, pl.ds(base + CELLS + 8, 8), :] = field[c, pl.ds(base + 9, 8), :]
        for n, (side, partner) in enumerate(x_links):
            if mode != "raw":
                added = combine([x_gain[n, j] for j in range(chips)], x_ends(message, n))
            for t in range(times):
                at = pl.ds(4 * t, 4)
                value = x_recv[message, n, at, :]
                if mode != "raw":
                    value = value + x_recv[power_message, n, at, :] * added
                value = finish(value, x_old, (c, n, at, slice(None)))
                field[c, pl.ds(t * TALL + side * (CELLS + 9), 4, stride=2), :] = value
        for n, (side, partner) in enumerate(y_links):
            if mode != "raw":
                added = combine([y_gain[n, j] for j in range(chips)], y_ends(message, n))
            for k in range(4):
                at = pl.ds(8 * k, times)
                value = y_recv[message, n, at, :]
                if mode != "raw":
                    value = value + y_recv[power_message, n, at, :] * added[k : k + 1]
                value = finish(value, y_old, (c, n, at, slice(None)))
                for i in range(8):
                    turned = pltpu.roll(
                        value, lax.rem(112 * (1 - side) + 128 - BLOCK_EDGE * i, 128), 1
                    )
                    row = ((k % 2) * 8 + i) * 8 + k // 2 + side * 6
                    ghost_y[c, pl.ds(row, times, stride=WIDE), :] = turned
        added = [None, None]
        for side in range(2):
            if mode != "raw":
                gains = [z_gain[side, j] for j in range(chips)]
                added[side] = combine(gains, z_ends(message, side))
        even = z_index % 2 == 0
        for t in range(times):
            at = pl.ds(8 * t, 8)
            pair = []
            for side in range(2):
                value = z_recv[message, side, at, :]
                if mode != "raw":
                    value = value + z_recv[power_message, side, at, :] * added[side]
                value = jnp.where((core != side) | outer_known, value, 0.0)
                pair.append(finish(value, z_old, (c, side, at, slice(None))))
            low, high = pair[0], pltpu.roll(pair[1], 15, 1)
            ghost_z[c, pl.ds(16 * t, 8), :] = jnp.where(even, low, high)
            ghost_z[c, pl.ds(16 * t + 8, 8), :] = jnp.where(even, high, low)

    def stencil(c, t, x, row, parity, factors):
        base = t * TALL + 8 + row

        def load(shift):
            return field[c, pl.ds(base + shift, 8), :]

        value = load(0)
        total = factors[0] * load(-8) + factors[1] * load(8)
        beyond = ghost_y[c, pl.ds(t * WIDE + row, 8), :]
        low = jnp.where(y_upper, load(-4), jnp.where(low_inner, load(2), beyond))
        low = pltpu.roll(jnp.where(last_block, low, value), 16, 1)
        high = jnp.where(y_upper, jnp.where(high_inner, load(-2), beyond), load(4))
        high = pltpu.roll(jnp.where(first_block, high, value), 112, 1)
        total = total + factors[2] * low + factors[3] * high
        edge = ghost_z[c, pl.ds(16 * t + 8 * parity, 8), :]
        edge = pltpu.roll(edge, lax.rem(128 - x, 128), 1)
        low = jnp.where(z_first, edge, pltpu.roll(value, 1, 1))
        high = jnp.where(z_last, edge, pltpu.roll(value, 127, 1))
        return value, total + factors[4] * low + factors[5] * high

    def over_planes(body, unroll=ONCE):
        def one(group, carry):
            for i in range(unroll):
                x = group * unroll + i
                body(x, pl.multiple_of(x * 8, 8), i % 2)
            return carry

        lax.fori_loop(0, PLANES // unroll, one, 0)

    def factors_at(row):
        return [coefficient[f, pl.ds(row, 8), :] for f in range(6)]

    def sweep(c):
        def plane(x, row, parity):
            factors = factors_at(row)
            ratio = power[pl.ds(row, 8), :]
            before = None
            for t in range(times):
                _, total = stencil(c, t, x, row, parity, factors)
                total = total + source[c, pl.ds(t * CELLS + row, 8), :]
                if before is not None:
                    total = total + ratio * before
                local_field[c, pl.ds(t * WIDE + row, 8), :] = total
                before = total
            end_send[c, pl.ds(row, 8), :] = before + carry[c, pl.ds(row, 8), :]

        over_planes(plane, UNROLL)

    def first_residual(c):
        def plane(x, row, parity):
            factors = factors_at(row)
            ratio = power[pl.ds(row, 8), :]
            inverse = scale[pl.ds(row, 8), :]
            alive = present[6]
            earlier = jnp.where(chip == 0, start[c, pl.ds(row, 8), :], 0.0)
            before = None
            for t in range(times):
                value, total = stencil(c, t, x, row, parity, factors)
                total = total + inverse * force[c, pl.ds(t * CELLS + row, 8), :]
                total = (total + (ratio * earlier - value)) * alive
                source[c, pl.ds(t * CELLS + row, 8), :] = total
                if before is not None:
                    total = total + ratio * before
                local_field[c, pl.ds(t * WIDE + row, 8), :] = total
                before, earlier = total, value
            kept_end = kept * (earlier * alive)
            carry[c, pl.ds(row, 8), :] = kept_end
            end_send[c, pl.ds(row, 8), :] = before + kept_end

        over_planes(plane)

    def complete(message, c, last):
        def plane(x, row, parity):
            ends = [end_recv[message, j, pl.ds(row, 8), :] for j in range(chips - 1)]
            ends.append(end_send[c, pl.ds(row, 8), :])
            gains = [gain[j, pl.ds(row, 8), :] for j in range(chips)]
            added = combine(gains, ends)
            if last:
                carry_in[c, pl.ds(row, 8), :] = added
            for t in range(times):
                value = local_field[c, pl.ds(t * WIDE + row, 8), :]
                value = value + power[pl.ds(t * WIDE + row, 8), :] * added
                at = pl.ds(t * TALL + 8 + row, 8)
                if last:
                    local_field[c, pl.ds(t * WIDE + row, 8), :] = value
                    value = value - field[c, at, :]
                field[c, at, :] = value

        over_planes(plane)

    def last_residual(c):
        def plane(x, row, parity):
            factors = factors_at(row)
            diagonal = 1.0 / scale[pl.ds(row, 8), :]
            for t in range(times):
                _, total = stencil(c, t, x, row, parity, factors)
                total = total * diagonal
                if t == 0:
                    added = carry_in[c, pl.ds(row, 8), :]
                    total = total - jnp.where(chip == 0, 2.0 * added, 0.0)
                source[c, pl.ds(t * CELLS + row, 8), :] = total

        over_planes(plane)

    def take(stage_ref, origin, store):
        for j in range(local):
            for q in range(half):
                store(origin * local + j, q, stage_ref[q, pl.ds(j, ROWS, stride=local), :])

    def scatter(value, target, q):
        target[pl.ds(q, ROWS, stride=half), :] = value

    for copy in smalls:
        copy.wait()
    for q in range(half):
        slot = core * half + q
        scatter(small_viscosity[:, slot, :], scale, q)
        for d in range(3):
            scatter(small_peclet[d, :, slot, :], coefficient.at[2 * d], q)
        for c in range(COMPONENTS):
            scatter(small_initial[c, :, slot, :], start.at[c], q)
    for f in range(7):
        value = jnp.zeros((8, LANES), jnp.float32)
        for q in range(half):
            slot = core * half + q
            known = live[slot] > 0 if f == 6 else holder[slot, f] >= 0
            value = jnp.where(slot_index == q, jnp.where(known, 1.0, 0.0), value)
        present[f] = value

    def make(x, row, parity):
        at = pl.ds(row, 8)
        thickness = scale[at, :]
        inverse = 1.0 / (2.0 + 6.0 * thickness)
        scale[at, :] = inverse
        weight = thickness * inverse
        edges = [
            x == 0,
            x == PLANES - 1,
            (~y_upper) & first_block,
            y_upper & last_block,
            z_first,
            z_last,
        ]
        for d in range(3):
            number = coefficient[2 * d, at, :]
            for f, factor in ((2 * d, 1.0 + number), (2 * d + 1, 1.0 - number)):
                slot_edge = edges[f]
                value = weight * factor
                coefficient[f, at, :] = jnp.where(slot_edge, value * present[f], value)
        ratio = 2.0 * inverse
        total = ratio
        for t in range(times):
            power[pl.ds(t * WIDE + row, 8), :] = total
            if t == times - 1:
                for j, value in enumerate(gains_of(total)):
                    gain[j, at, :] = value
            total = total * ratio

    over_planes(make)
    ghost_y[...] = jnp.zeros_like(ghost_y)

    pack(power_message, lambda at: power[at, :], WIDE, 0)
    power_last = (times - 1) * WIDE
    pack_last(power_message, lambda at: power[pl.ds(power_last + at.start, at.size, at.stride), :])

    def offer(c):
        for copy in owns(c):
            copy.wait()

        def store_both(t, q, value):
            field[c, pl.ds(t * TALL + 8 + q, ROWS, stride=half), :] = value
            local_field[c, pl.ds(t * WIDE + q, ROWS, stride=half), :] = value

        def store_away(t, q, value):
            local_field[c, pl.ds(t * WIDE + q, ROWS, stride=half), :] = value

        take(stage_iterate.at[core, :, c], core, store_both)
        take(stage_away.at[:, c], 1 - core, store_away)
        pack(c, lambda at: local_field[c, at, :], WIDE, 0, split=True)

    offer(0)
    pl.semaphore_wait(barrier, len(greet))
    start_first(0)
    for c in range(COMPONENTS):
        for copy in swaps(c):
            copy.start()
    power_copies = halos(power_message)
    start_all(power_copies)

    def offering(c, carry):
        offer(c)
        start_first(c)
        return carry

    lax.fori_loop(1, COMPONENTS, offering, 0)

    def send_local(message, c):
        pack_last(message, lambda at: end_send[c, at, :])
        start_all(faces(message))
        start_all(carries(message, c))
        found = halos(message)
        first, second = len(x_links), len(x_links) + len(y_links)

        def load(at):
            return local_field[c, at, :]

        pack_z(message, load, WIDE, 0)
        start_all(found[second:])
        pack_y(message, load, WIDE, 0)
        start_all(found[first:second])
        pack_x(message, load, WIDE, 0)
        start_all(found[:first])

    def opening(c, carry):
        for copy in swaps(c):
            copy.wait()
        own_forcing(c).wait()

        def store(t, q, value):
            field[c, pl.ds(t * TALL + 8 + q, ROWS, stride=half), :] = value

        def store_force(t, q, value):
            force[c, pl.ds(t * CELLS + q, ROWS, stride=half), :] = value

        take(stage_iterate.at[1 - core, :, c], 1 - core, store)
        for origin in range(2):
            take(stage_forcing.at[origin, :, c], origin, store_force)
        wait_first(c)
        ghosts(c, c, "raw")
        first_residual(c)
        send_local(COMPONENTS + c, c)
        return carry

    lax.fori_loop(0, COMPONENTS, opening, 0)
    wait_all(power_copies)
    for n in range(len(x_links)):
        for j, value in enumerate(gains_of(x_recv[power_message, n, pl.ds(4 * times, 4), :])):
            x_gain[n, j] = value
    for n in range(len(y_links)):
        for j, value in enumerate(gains_of(y_recv[power_message, n, pl.ds(32, 4), :])):
            y_gain[n, j] = value
    for side in range(2):
        ratio = z_recv[power_message, side, pl.ds(8 * times, 8), :]
        for j, value in enumerate(gains_of(ratio)):
            z_gain[side, j] = value

    def turn(step, carry):
        c = lax.rem(step, COMPONENTS)
        message = COMPONENTS + step
        wait_all(halos(message))
        wait_all(faces(message))
        wait_all(carries(message, c))
        complete(message, c, False)
        ghosts(message, c, "next")
        sweep(c)
        send_local(message + COMPONENTS, c)
        return carry

    lax.fori_loop(0, COMPONENTS * (SWEEPS - 1), turn, 0)

    def giving(c, stage_ref, out, number):
        away = remote(
            stage_ref.at[1 - core, :, c], out.at[mine, c], stage, number + c, peer
        )
        here = pltpu.make_async_copy(
            stage_ref.at[core, :, c], out.at[mine, c], stage_local.at[number + c]
        )
        return [away, here]

    def fill(c, stage_ref, load, added):
        for origin in range(2):
            for j in range(local):
                for q in range(half):
                    value = load(origin * local + j, q)
                    at = pl.ds(j, ROWS, stride=local)
                    if added:
                        value = value + stage_ref[origin, q, c, at, :]
                    stage_ref[origin, q, c, at, :] = value

    gives = ((stage_iterate, out_velocity, 2 * COMPONENTS), (stage_forcing, out_residual, 3 * COMPONENTS))

    def closing(c, carry):
        message = COMPONENTS * SWEEPS + c
        wait_all(carries(message, c))
        complete(message, c, True)
        fill(
            c,
            stage_iterate,
            lambda t, q: local_field[c, pl.ds(t * WIDE + q, ROWS, stride=half), :],
            True,
        )
        for copy in giving(c, *gives[0]):
            copy.start()
        wait_all(halos(message))
        wait_all(faces(message))
        ghosts(message, c, "last")
        last_residual(c)
        fill(
            c,
            stage_forcing,
            lambda t, q: source[c, pl.ds(t * CELLS + q, ROWS, stride=half), :],
            False,
        )
        for copy in giving(c, *gives[1]):
            copy.start()
        return carry

    lax.fori_loop(0, COMPONENTS, closing, 0)
    for c in range(COMPONENTS):
        for give in gives:
            for copy in giving(c, *give):
                copy.wait()


def emit(first, second, first_out, second_out, sem):
    copies = [
        pltpu.make_async_copy(first, first_out, sem.at[0]),
        pltpu.make_async_copy(second, second_out, sem.at[1]),
    ]
    for copy in copies:
        copy.start()
    for copy in copies:
        copy.wait()


def body(
    iterate,
    forcing,
    initial_velocity,
    viscosity,
    peclet,
    live_patch_mask,
    neighbour_holder,
    neighbour_slot,
):
    time_devices = lax.axis_size("tm")
    chips = time_devices // 2
    levels = lax.axis_size("space").bit_length() - 1
    slots, local = iterate.shape[:2]
    half = slots // 2
    times = 2 * local

    def by_rows(array):
        split = array.reshape(array.shape[:-1] + (ROWS, LANES))
        if split.ndim == 4:
            return split.transpose(1, 2, 0, 3)
        split = split.transpose(0, 2, 3, 1, 4)
        return split.reshape(slots, COMPONENTS, ROWS * local, LANES)

    def whole(array):
        split = array.reshape(slots, COMPONENTS, ROWS, local, LANES)
        return split.transpose(0, 3, 1, 2, 4).reshape(slots, local, COMPONENTS, ROWS * LANES)

    count = [len(range(d, levels, 3)) for d in range(3)]
    messages = COMPONENTS * (SWEEPS + 1) + 1
    per_message = (chips - 1) + chips * (count[0] + count[1] + 1 + count[2])
    others = max(chips - 1, 1)
    f32 = jnp.float32
    stage = pltpu.VMEM((2, half, COMPONENTS, ROWS * local, LANES), f32)

    def rows(*shape):
        return pltpu.VMEM(shape + (LANES,), f32)

    nx, ny = max(count[0], 1), max(count[1], 1)
    x_rows, y_rows, z_rows = 4 * times + 8, 40, 8 * times + 8
    result = pltpu.VMEM((slots, COMPONENTS, ROWS * local, LANES), f32)
    velocity, residual = pl.pallas_call(
        functools.partial(kernel, (chips, levels, slots, local)),
        out_shape=(result, result),
        in_specs=[pl.BlockSpec(memory_space=pltpu.SMEM)] * 2
        + [pl.BlockSpec(memory_space=pl.ANY)] * 5,
        out_specs=[pl.BlockSpec(memory_space=pl.ANY)] * 2,
        scratch_shapes=[
            stage,
            stage,
            pltpu.VMEM((half, COMPONENTS, ROWS * local, LANES), f32),
            rows(COMPONENTS, times * TALL),
            rows(COMPONENTS, times * WIDE),
            rows(COMPONENTS, times * CELLS),
            rows(COMPONENTS, times * CELLS),
            rows(COMPONENTS, CELLS),
            rows(COMPONENTS, ROWS, slots),
            rows(ROWS, slots),
            rows(COMPONENTS, ROWS, slots),
            rows(COMPONENTS, times * WIDE),
            rows(COMPONENTS, times * 16),
            rows(6, CELLS),
            rows(times * WIDE),
            rows(CELLS),
            rows(chips, CELLS),
            rows(COMPONENTS, CELLS),
            rows(COMPONENTS, CELLS),
            rows(COMPONENTS, CELLS),
            rows(7, 8),
            rows(messages, nx, x_rows),
            rows(messages, nx, x_rows),
            rows(messages, ny, y_rows),
            rows(messages, ny, y_rows),
            rows(messages, 2, z_rows),
            rows(messages, 2, z_rows),
            rows(messages, nx, 4),
            rows(messages, ny, 4),
            rows(COMPONENTS, ny, 2, 4 * local),
            rows(COMPONENTS, ny, 2, 4 * local),
            rows(messages, nx, others, 4),
            rows(messages, ny, others, 4),
            rows(messages, 2, others, 8),
            rows(messages, others, CELLS),
            rows(nx, chips, 4),
            rows(ny, chips, 4),
            rows(2, chips, 8),
            rows(COMPONENTS, nx, x_rows),
            rows(COMPONENTS, ny, y_rows),
            rows(COMPONENTS, 2, z_rows),
            pltpu.SemaphoreType.DMA((messages * per_message,)),
            pltpu.SemaphoreType.DMA((messages * per_message,)),
            pltpu.SemaphoreType.DMA((4 * COMPONENTS,)),
            pltpu.SemaphoreType.DMA((4 * COMPONENTS,)),
            pltpu.SemaphoreType.DMA((4 * COMPONENTS,)),
            pltpu.SemaphoreType.DMA((COMPONENTS,)),
            pltpu.SemaphoreType.DMA((3,)),
        ],
        compiler_params=pltpu.CompilerParams(
            collective_id=0, has_side_effects=True, vmem_limit_bytes=121 * 512 * 1024
        ),
    )(
        neighbour_holder,
        live_patch_mask,
        by_rows(iterate),
        by_rows(forcing),
        by_rows(initial_velocity),
        viscosity.reshape(slots, ROWS, LANES).transpose(1, 0, 2),
        by_rows(peclet),
    )
    shape = jax.ShapeDtypeStruct((slots, COMPONENTS, ROWS * local, LANES), f32)
    velocity = pltpu.with_memory_space_constraint(velocity, pltpu.MemorySpace.VMEM)
    residual = pltpu.with_memory_space_constraint(residual, pltpu.MemorySpace.VMEM)
    velocity, residual = pl.pallas_call(
        emit,
        out_shape=(shape, shape),
        in_specs=[pl.BlockSpec(memory_space=pltpu.MemorySpace.VMEM)] * 2,
        out_specs=[pl.BlockSpec(memory_space=pl.ANY)] * 2,
        scratch_shapes=[pltpu.SemaphoreType.DMA((2,))],
        compiler_params=pltpu.CompilerParams(vmem_limit_bytes=4 * 1024 * 1024),
    )(velocity, residual)
    return whole(velocity), whole(residual)


def solution(mesh):
    return jax.shard_map(
        body,
        mesh=mesh,
        in_specs=(
            P("space", "tm", None, None),
            P("space", "tm", None, None),
            P("space", None, None),
            P("space", None),
            P("space", None, None),
            P("space"),
            P("space", None),
            P("space", None),
        ),
        out_specs=(P("space", "tm", None, None), P("space", "tm", None, None)),
        check_vma=False,
    )
```
